256 devices in a mesh: group: 32 (over x_hi, z, core), tensor: 8 (over y, x_lo).
Axes of the slice: x: 4 (x_hi: 2, x_lo: 2; x = x_hi * 2 + x_lo), y: 4, z: 8, core: 2. Of those that a mesh axis runs over, the one named last changes fastest.
Arguments:
- hidden: bfloat16 [64, 16384], P('group'), may hold values from -6 to 6
- norm_gain: float32 [16384], replicated, may hold values from 0.1 to 1.9
- slab_of: int32 [32], replicated, may hold values from 0 to 31, each once
- w_query: bfloat16 [16384, 16384], P('group', 'tensor'), may hold values from -0.046875 to 0.046875
- w_key: bfloat16 [16384, 1024], P('group', 'tensor'), may hold values from -0.046875 to 0.046875
- w_value: bfloat16 [16384, 1024], P('group', 'tensor'), may hold values from -0.046875 to 0.046875
- w_out: bfloat16 [16384, 16384], P('tensor', 'group'), may hold values from -0.046875 to 0.046875
- k_cache: bfloat16 [64, 8, 4096, 128], P('group', 'tensor'), may hold values from -1000 to 1000
- v_cache: bfloat16 [64, 8, 4096, 128], P('group', 'tensor'), may hold values from -6 to 6
- lengths: int32 [64], P('group'), may hold values from 1 to 4096, as said below
Outputs:
- out_hidden: bfloat16 [64, 16384], P('group')
- new_keys: bfloat16 [64, 8, 128], P('group', 'tensor')
- new_values: bfloat16 [64, 8, 128], P('group', 'tensor')
The draws below stay inside these ranges and needn't reach their ends.
Inputs may be any that keep to these rules, and one draw needn't show every extreme that they name: `lengths`: some sequence holds exactly 4096 cached positions.
All inputs are finite; a program needn't handle non-finite values.
Results may differ from the reference program's by a relative error of at most 0.0085.
Values may be sent and summed in bfloat16 or wider, within the bound.
No kernel may reach another device: no remote copies, remote signals or barrier semaphores. Data moves between devices by JAX's collectives and lax.ppermute only.
A program may use at most 64 MiB of HBM per device.

```python
import math
import jax
import jax.numpy as jnp
from jax import lax

D = 16384
HEADS = 128
KV_HEADS = 8
HEAD_DIM = 128
CACHE = 4096
BATCH = 64
SLABS = 32
N_GROUP = 32


def draw_lengths(key, part):
    key = jax.random.fold_in(key, 11)
    first_key, second_key = jax.random.split(key)
    values = jax.random.randint(first_key, (BATCH,), 1, CACHE + 1)
    where_full = jax.random.randint(second_key, (), 0, BATCH)
    return values.at[where_full].set(CACHE).astype(jnp.int32)


def draw_k_cache(key, part):
    key = jax.random.fold_in(key, 23)
    base_key = jax.random.fold_in(key, 0)
    shape = (BATCH, KV_HEADS, CACHE, HEAD_DIM)
    base = jnp.clip(jax.random.normal(base_key, shape, jnp.float32), -6.0, 6.0)
    return base.astype(jnp.bfloat16)


def shard_levels(rng, shape, shards, least, largest):
    def one(dim, parts):
        draws = jax.random.uniform(jax.random.fold_in(jax.random.fold_in(rng, 6), dim), (parts,), jnp.float32, least / len(shards), largest / len(shards))
        return jnp.repeat(jnp.exp(draws), shape[dim] // parts).reshape((-1,) + (1,) * (len(shape) - dim - 1))

    gain = one(*shards[0])
    for cut in shards[1:]:
        gain = gain * one(*cut)
    return gain


def normal_values(own_key, dims, spread, most, cuts=(), kind=jnp.bfloat16):
    level = shard_levels(own_key, dims, cuts, -0.22, 0.18) if cuts else 1.0
    entries = jax.random.normal(own_key, dims, jnp.float32) * spread * level
    return jnp.minimum(jnp.maximum(entries, -most), most).astype(kind)


def setup_inputs(seed: int = 0) -> dict:
    splits = jax.random.split(jax.random.key(seed), 11)
    hidden = normal_values(splits[0], (BATCH, D), 1.0, 6.0, ((0, 32),))
    norm_gain = jnp.clip(1.0 + 0.18 * jax.random.normal(splits[1], (D,), jnp.float32), 0.1, 1.9)
    slab_of = jax.random.permutation(splits[2], SLABS).astype(jnp.int32)
    w_query = normal_values(splits[3], (D, HEADS * HEAD_DIM), D ** -0.5, 0.046875, ((0, 32), (1, 8)))
    w_key = normal_values(splits[4], (D, KV_HEADS * HEAD_DIM), D ** -0.5, 0.046875, ((0, 32), (1, 8)))
    w_value = normal_values(splits[5], (D, KV_HEADS * HEAD_DIM), D ** -0.5, 0.046875, ((0, 32), (1, 8)))
    w_out = normal_values(splits[6], (HEADS * HEAD_DIM, D), (HEADS * HEAD_DIM) ** -0.5, 0.046875, ((0, 8), (1, 32)))
    k_cache = draw_k_cache(jax.random.fold_in(splits[10], 71), 0)
    v_cache = normal_values(splits[8], (BATCH, KV_HEADS, CACHE, HEAD_DIM), 1.0, 6.0, ((0, 32), (1, 8)))
    lengths = draw_lengths(jax.random.fold_in(splits[10], 71), 0)
    return dict(hidden=hidden, norm_gain=norm_gain, slab_of=slab_of, w_query=w_query, w_key=w_key, w_value=w_value, w_out=w_out, k_cache=k_cache, v_cache=v_cache, lengths=lengths)


def rotate(values, angles):
    half_dim = values.shape[-1] // 2
    cosine = jnp.cos(angles)
    sine_part = jnp.sin(angles)
    first_half = values[..., :half_dim]
    second_half = values[..., half_dim:]
    return jnp.concatenate([first_half * cosine - second_half * sine_part, second_half * cosine + first_half * sine_part], axis=-1)

def angles_for(lengths, head_dim):
    half_dim = head_dim // 2
    frequency = jnp.exp(-math.log(500000.0) * (2.0 * jnp.arange(half_dim, dtype=jnp.float32)) / head_dim)
    return lengths.astype(jnp.float32)[:, None] * frequency[None, :]

def attend_one(inputs):
    scaled, keys_cached, values_cached, key_new, value_new, length = inputs
    scores = jnp.einsum('grd,gld->grl', scaled.astype(jnp.float32), keys_cached.astype(jnp.float32))
    own_score = jnp.einsum('grd,gd->gr', scaled.astype(jnp.float32), key_new.astype(jnp.float32))
    visible = (jnp.arange(keys_cached.shape[1]) < length)[None, None, :]
    masked = jnp.where(visible, scores, -1e+30)
    highest = jnp.maximum(lax.optimization_barrier(jnp.max(masked, axis=-1)), own_score)
    exponent = jnp.where(visible, jnp.exp(masked - highest[..., None]), 0.0)
    own_exp = jnp.exp(own_score - highest)
    denominator = lax.optimization_barrier(jnp.sum(exponent, axis=-1)) + own_exp
    weights = (exponent / denominator[..., None]).astype(jnp.bfloat16)
    own_weight = (own_exp / denominator).astype(jnp.bfloat16)
    combined = jnp.einsum('grl,gld->grd', weights.astype(jnp.float32), values_cached.astype(jnp.float32))
    combined = combined + own_weight.astype(jnp.float32)[..., None] * value_new.astype(jnp.float32)[:, None, :]
    return combined.astype(jnp.bfloat16)

def reference(hidden, norm_gain, slab_of, w_query, w_key, w_value, w_out, k_cache, v_cache, lengths):
    slab_width = D // N_GROUP
    inverse = jnp.argsort(slab_of).astype(jnp.int32)

    def true_rows(weight):
        return weight.reshape(N_GROUP, slab_width, weight.shape[1])[inverse].reshape(D, weight.shape[1])
    true_out = w_out.reshape(w_out.shape[0], N_GROUP, slab_width)[:, inverse].reshape(w_out.shape[0], D)
    hidden_wide = hidden.astype(jnp.float32)
    mean_square = lax.optimization_barrier(jnp.mean(hidden_wide * hidden_wide, axis=1, keepdims=True))
    normed = (hidden_wide * lax.rsqrt(mean_square + 1e-05) * norm_gain).astype(jnp.bfloat16)
    queries = jnp.dot(normed, true_rows(w_query), preferred_element_type=jnp.float32).reshape(BATCH, HEADS, HEAD_DIM)
    keys_new = jnp.dot(normed, true_rows(w_key), preferred_element_type=jnp.float32).reshape(BATCH, KV_HEADS, HEAD_DIM)
    values_new = jnp.dot(normed, true_rows(w_value), preferred_element_type=jnp.float32).reshape(BATCH, KV_HEADS, HEAD_DIM)
    angles = angles_for(lengths, HEAD_DIM)[:, None, :]
    new_keys = rotate(keys_new, angles).astype(jnp.bfloat16)
    new_values = values_new.astype(jnp.bfloat16)
    group_ratio = HEADS // KV_HEADS
    scaled = (rotate(queries, angles) / math.sqrt(HEAD_DIM)).astype(jnp.bfloat16).reshape(BATCH, KV_HEADS, group_ratio, HEAD_DIM)
    attended = lax.map(attend_one, (scaled, k_cache, v_cache, new_keys, new_values, lengths))
    attended = attended.reshape(BATCH, HEADS * HEAD_DIM)
    projection = jnp.dot(attended, true_out, preferred_element_type=jnp.float32)
    out_hidden = (hidden_wide + projection).astype(jnp.bfloat16)
    return (out_hidden, new_keys, new_values)
```

```python
import math

import jax
import jax.numpy as jnp
from jax import lax
from jax.sharding import PartitionSpec as P

ROTARY_BASE = 500000.0


def rotate(values, angles):
    half_dim = values.shape[-1] // 2
    cosine = jnp.cos(angles)
    sine_part = jnp.sin(angles)
    first_half = values[..., :half_dim]
    second_half = values[..., half_dim:]
    return jnp.concatenate(
        [
            first_half * cosine - second_half * sine_part,
            second_half * cosine + first_half * sine_part,
        ],
        axis=-1,
    )


def angles_for(lengths, head_dim):
    half_dim = head_dim // 2
    frequency = jnp.exp(
        -math.log(ROTARY_BASE) * (2.0 * jnp.arange(half_dim, dtype=jnp.float32)) / head_dim
    )
    return lengths.astype(jnp.float32)[:, None] * frequency[None, :]


def exchange(tiles, axis, sets):
    return lax.all_to_all(tiles, axis, 0, 0, tiled=True, axis_index_groups=sets)


def attend(projected, k_cache, v_cache, lengths, query_cols, key_cols):
    sequences = projected.shape[0]
    head_dim = k_cache.shape[3]
    kv_local = k_cache.shape[1]
    queries = projected[:, :query_cols].reshape(sequences, query_cols // head_dim, head_dim)
    keys_new = projected[:, query_cols : query_cols + key_cols].reshape(
        sequences, kv_local, head_dim
    )
    values_new = projected[:, query_cols + key_cols :].reshape(sequences, kv_local, head_dim)
    angles = angles_for(lengths, head_dim)[:, None, :]
    new_keys = rotate(keys_new, angles).astype(jnp.bfloat16)
    new_values = values_new.astype(jnp.bfloat16)
    group_ratio = queries.shape[1] // kv_local
    scaled = (
        (rotate(queries, angles) / math.sqrt(head_dim))
        .astype(jnp.bfloat16)
        .reshape(sequences, kv_local, group_ratio, head_dim)
    )
    scores = jnp.einsum("bgrd,bgld->bgrl", scaled, k_cache, preferred_element_type=jnp.float32)
    own_score = jnp.einsum("bgrd,bgd->bgr", scaled, new_keys, preferred_element_type=jnp.float32)
    visible = (jnp.arange(k_cache.shape[2])[None, :] < lengths[:, None])[:, None, None, :]
    masked = jnp.where(visible, scores, -1e30)
    highest = jnp.maximum(jnp.max(masked, axis=-1), own_score)
    exponent = jnp.where(visible, jnp.exp(masked - highest[..., None]), 0.0)
    own_exp = jnp.exp(own_score - highest)
    denominator = jnp.sum(exponent, axis=-1) + own_exp
    weights = (exponent / denominator[..., None]).astype(jnp.bfloat16)
    own_weight = (own_exp / denominator).astype(jnp.bfloat16)
    combined = jnp.einsum("bgrl,bgld->bgrd", weights, v_cache, preferred_element_type=jnp.float32)
    combined = (
        combined
        + own_weight.astype(jnp.float32)[..., None] * new_values.astype(jnp.float32)[:, :, None, :]
    )
    attended = combined.astype(jnp.bfloat16).reshape(sequences, query_cols)
    return attended, new_keys, new_values


def solution(mesh):
    groups = mesh.shape["group"]
    tensors = mesh.shape["tensor"]
    chips = groups // 2
    half = chips // 2
    partner = [(i, i ^ 1) for i in range(groups)]
    same_core = [[2 * chip + core for chip in range(chips)] for core in range(2)]
    near = [
        [
            (2 * chip + core) * tensors + (pair * 2 + ((chip // half) ^ side))
            for chip in range(chips)
        ]
        for core in range(2)
        for pair in range(tensors // 2)
        for side in range(2)
    ]

    def body(
        hidden, norm_gain, slab_of, w_query, w_key, w_value, w_out, k_cache, v_cache, lengths
    ):
        sequences, model_width = hidden.shape
        slab_width = model_width // groups
        core = lax.axis_index("group") % 2
        other_query, other_key, other_value, other_out = (
            lax.ppermute(w, "group", partner) for w in (w_query, w_key, w_value, w_out)
        )
        order = slab_of.reshape(chips, 2)
        order = jnp.where(core == 0, order, order[:, ::-1]).reshape(-1)
        hidden_wide = hidden.astype(jnp.float32)
        mean_square = jnp.mean(hidden_wide * hidden_wide, axis=1, keepdims=True)
        normed = (hidden_wide * lax.rsqrt(mean_square + 1e-05) * norm_gain).astype(jnp.bfloat16)
        arranged = jnp.take(normed.reshape(sequences, groups, slab_width), order, axis=1)
        arranged = jnp.swapaxes(arranged.reshape(sequences, chips, 2 * slab_width), 0, 1)
        columns = exchange(arranged, ("group", "tensor"), near).reshape(
            chips * sequences, 2 * slab_width
        )
        own, other = columns[:, :slab_width], columns[:, slab_width:]

        def project(w, w_other):
            return jnp.dot(own, w, preferred_element_type=jnp.float32) + jnp.dot(
                other, w_other, preferred_element_type=jnp.float32
            )

        partial = jnp.concatenate(
            [
                project(w_query, other_query),
                project(w_key, other_key),
                project(w_value, other_value),
            ],
            axis=1,
        ).reshape(chips, sequences, -1)
        projected = exchange(partial, "group", same_core).sum(axis=0)
        attended, new_keys, new_values = attend(
            projected, k_cache, v_cache, lengths, w_query.shape[1], w_key.shape[1]
        )
        gathered = exchange(
            jnp.broadcast_to(attended[None], (chips, *attended.shape)), "group", same_core
        ).reshape(chips * sequences, -1)
        head_partial = jnp.concatenate(
            [
                jnp.dot(gathered, w_out, preferred_element_type=jnp.float32),
                jnp.dot(gathered, other_out, preferred_element_type=jnp.float32),
            ],
            axis=1,
        ).astype(jnp.bfloat16)
        returned = exchange(
            head_partial.reshape(chips, sequences, 2 * slab_width), "group", same_core
        )
        everyone = lax.all_to_all(
            jnp.broadcast_to(returned[None], (tensors, *returned.shape)), "tensor", 0, 0, tiled=True
        )
        summed = jnp.sum(everyone.astype(jnp.float32), axis=0)
        summed = jnp.swapaxes(summed, 0, 1).reshape(sequences, groups, slab_width)
        ordered = jnp.take(summed, jnp.argsort(order), axis=1).reshape(sequences, model_width)
        out_hidden = (hidden_wide + ordered).astype(jnp.bfloat16)
        return (out_hidden, new_keys, new_values)

    in_specs = (
        P("group", None),
        P(),
        P(),
        P("group", "tensor"),
        P("group", "tensor"),
        P("group", "tensor"),
        P("tensor", "group"),
        P("group", "tensor", None, None),
        P("group", "tensor", None, None),
        P("group"),
    )
    out_specs = (P("group", None), P("group", "tensor", None), P("group", "tensor", None))
    return jax.shard_map(body, mesh=mesh, in_specs=in_specs, out_specs=out_specs, check_vma=False)
```

```python
import functools
import math

import jax
import jax.numpy as jnp
from jax import lax
from jax.experimental import pallas as pl
from jax.experimental.pallas import tpu as pltpu
from jax.sharding import PartitionSpec as P

ROTARY_BASE = 500000.0
EPSILON = 1e-05
LANES = 128
WIDE = jnp.float32
NARROW = jnp.bfloat16


def in_vmem(*arrays):
    return [pltpu.with_memory_space_constraint(a, pltpu.VMEM) for a in arrays]


def in_hbm(*arrays):
    return [pltpu.with_memory_space_constraint(a, pltpu.HBM) for a in arrays]


def call(kernel, outs, scalars, arrays, scratch=(), far=(), **sizes):
    def at(space, operands):
        return [pl.BlockSpec(memory_space=space)] * len(operands)

    return pl.pallas_call(
        functools.partial(kernel, **sizes),
        out_shape=outs,
        in_specs=at(pltpu.SMEM, scalars) + at(pltpu.HBM, far) + at(pltpu.VMEM, arrays),
        out_specs=jax.tree.map(lambda _: pl.BlockSpec(memory_space=pltpu.VMEM), outs),
        scratch_shapes=list(scratch),
        compiler_params=pltpu.CompilerParams(vmem_limit_bytes=8 * 1024 * 1024),
        name=kernel.__name__,
    )(*scalars, *in_hbm(*far), *arrays)


def arrange(core_ref, *refs, slab):
    far, refs = refs[:7], refs[7:]
    out_ref, cos_ref, sin_ref, *kept, slab_ref, length_ref, hidden_ref, gain_ref, rows_ref, sems = refs
    near = (hidden_ref, gain_ref, slab_ref, length_ref, *kept)
    copies = [pltpu.make_async_copy(f, n, sems.at[i]) for i, (f, n) in enumerate(zip(far, near))]
    for copy in copies:
        copy.start()
    copies, later = copies[:4], copies[4:]
    sequences, width = hidden_ref.shape
    head_dim = cos_ref.shape[1]
    core = core_ref[0]
    lane = lax.broadcasted_iota(jnp.int32, (1, head_dim), 1)
    half_dim = head_dim // 2
    place_in_half = jnp.where(lane < half_dim, lane, lane - half_dim).astype(WIDE)
    frequency = jnp.exp(-math.log(ROTARY_BASE) * (2.0 * place_in_half) / head_dim)
    for copy in copies:
        copy.wait()
    squares = jnp.zeros((sequences, slab), WIDE)
    for first in range(0, width, slab):
        x = hidden_ref[:, first : first + slab].astype(WIDE)
        squares = squares + x * x
    scale = lax.rsqrt(jnp.sum(squares, axis=1, keepdims=True) / width + EPSILON)
    chips, lines = out_ref.shape[:2]
    pieces = slab // LANES
    for chip in range(chips):
        for place in range(2):
            index = 2 * chip + (core if place == 0 else 1 - core)
            first = pl.multiple_of(slab_ref[index] * slab, slab)
            x = hidden_ref[:, pl.ds(first, slab)].astype(WIDE)
            x = x * scale * gain_ref[:, pl.ds(first, slab)]
            for piece in range(pieces):
                line = chip * lines + place * pieces + piece
                rows_ref[pl.ds(line, sequences, stride=lines // sequences), :] = x[
                    :, piece * LANES : (piece + 1) * LANES
                ]
    for chip in range(chips):
        out_ref[chip] = rows_ref[chip * lines : (chip + 1) * lines, :].astype(NARROW)
    for s in range(sequences):
        angle = length_ref[s].astype(WIDE) * frequency
        cos_ref[s : s + 1, :] = jnp.cos(angle)
        sine = jnp.sin(angle)
        sin_ref[s : s + 1, :] = jnp.where(lane < half_dim, -sine, sine)
    for copy in later:
        copy.wait()


def rows_of(x_ref, wide_ref, pieces):
    sources, lines = x_ref.shape[:2]
    for source in range(sources):
        wide_ref[source * lines : (source + 1) * lines, :] = x_ref[source].astype(WIDE)
    rows = sources * lines // pieces
    return jnp.concatenate(
        [wide_ref[pl.ds(p, rows, stride=pieces), :].astype(NARROW) for p in range(pieces)], axis=1
    )


def project(x_ref, *refs, chunk):
    *weights, out_ref, wide_ref = refs
    depth = weights[0].shape[0]
    x = rows_of(x_ref, wide_ref, 2 * depth // LANES)
    own, other = x[:, :depth], x[:, depth:]
    rows = out_ref.shape[1]
    offset = 0
    for mine, partners in zip(weights[0::2], weights[1::2]):
        step = min(chunk, mine.shape[1])
        for first in range(0, mine.shape[1], step):
            part = jnp.dot(own, mine[:, first : first + step], preferred_element_type=WIDE)
            part += jnp.dot(other, partners[:, first : first + step], preferred_element_type=WIDE)
            for chip in range(out_ref.shape[0]):
                out_ref[chip, :, offset : offset + step] = part[chip * rows : (chip + 1) * rows]
            offset += step


def attend(
    length_ref, part_ref, cos_ref, sin_ref, k_ref, v_ref, out_ref, key_ref, value_ref, heads_ref,
    *, heads
):
    sequences = part_ref.shape[1]
    head_dim = k_ref.shape[3]
    cached = k_ref.shape[2]
    total = part_ref[0]
    for source in range(1, part_ref.shape[0]):
        total = total + part_ref[source]
    for s in range(sequences):
        for h in range(heads + 2):
            heads_ref[s, h : h + 1, :] = total[s : s + 1, h * head_dim : (h + 1) * head_dim]
    value_ref[...] = total[:, (heads + 1) * head_dim :].astype(NARROW)
    new_keys = []
    for s in range(sequences):
        cosine, sine = cos_ref[s : s + 1], sin_ref[s : s + 1]

        def rotate(x):
            return x * cosine + pltpu.roll(x, head_dim // 2, 1) * sine

        query = rotate(heads_ref[s, :heads, :])
        scaled = (query / math.sqrt(head_dim)).astype(NARROW)
        new_key = rotate(heads_ref[s, heads : heads + 1, :]).astype(NARROW)
        new_value = heads_ref[s, heads + 1 : heads + 2, :].astype(NARROW)
        new_keys.append(new_key.astype(WIDE))
        scores = lax.dot_general(
            scaled, k_ref[s, 0], (((1,), (1,)), ((), ())), preferred_element_type=WIDE
        )
        own_score = jnp.sum(scaled.astype(WIDE) * new_key.astype(WIDE), axis=1, keepdims=True)
        visible = lax.broadcasted_iota(jnp.int32, (heads, cached), 1) < length_ref[s]
        masked = jnp.where(visible, scores, -1e30)
        highest = jnp.maximum(jnp.max(masked, axis=1, keepdims=True), own_score)
        exponent = jnp.where(visible, jnp.exp(masked - highest), 0.0)
        own_exp = jnp.exp(own_score - highest)
        share = 1.0 / (jnp.sum(exponent, axis=1, keepdims=True) + own_exp)
        weights = (exponent * share).astype(NARROW)
        own_weight = (own_exp * share).astype(NARROW)
        combined = jnp.dot(weights, v_ref[s, 0], preferred_element_type=WIDE)
        combined = combined + own_weight.astype(WIDE) * new_value.astype(WIDE)
        attended = combined.astype(NARROW)
        for target in range(out_ref.shape[0]):
            out_ref[target, s * heads : (s + 1) * heads, :] = attended
    key_ref[...] = jnp.concatenate(new_keys, axis=0).astype(NARROW)


def project_out(x_ref, w_ref, other_ref, out_ref, rows_ref, parts_ref, *, heads):
    chips, lines = out_ref.shape[:2]
    x = rows_of(x_ref, rows_ref, heads)
    rows = x.shape[0]
    slab = w_ref.shape[1]
    pieces = slab // LANES
    for place, w in enumerate((w_ref, other_ref)):
        part = jnp.dot(x, w[...], preferred_element_type=WIDE)
        for piece in range(pieces):
            parts_ref[pl.ds(place * pieces + piece, rows, stride=2 * pieces), :] = part[
                :, piece * LANES : (piece + 1) * LANES
            ]
    for chip in range(chips):
        out_ref[chip] = parts_ref[chip * lines : (chip + 1) * lines, :].astype(NARROW)


def repeat(x_ref, out_ref):
    for chip in range(x_ref.shape[0]):
        x = x_ref[chip]
        for target in range(out_ref.shape[0]):
            out_ref[target, chip] = x


def finish(core_ref, slab_ref, parts_ref, hidden_ref, out_ref, sums_ref, *, slab):
    core = core_ref[0]
    chips, lines = parts_ref.shape[1:3]
    sequences = hidden_ref.shape[0]
    pieces = slab // LANES
    for chip in range(chips):
        total = parts_ref[0, chip].astype(WIDE)
        for source in range(1, parts_ref.shape[0]):
            total = total + parts_ref[source, chip].astype(WIDE)
        sums_ref[chip * lines : (chip + 1) * lines, :] = total
    for chip in range(chips):
        for place in range(2):
            index = 2 * chip + (core if place == 0 else 1 - core)
            first = slab_ref[index] * slab
            for piece in range(pieces):
                line = chip * lines + place * pieces + piece
                added = sums_ref[pl.ds(line, sequences, stride=lines // sequences), :]
                at = pl.ds(pl.multiple_of(first + piece * LANES, LANES), LANES)
                out_ref[:, at] = (hidden_ref[:, at].astype(WIDE) + added).astype(NARROW)


def exchange(tiles, axis, sets):
    return lax.all_to_all(tiles, axis, 0, 0, tiled=True, axis_index_groups=sets)


def solution(mesh):
    groups = mesh.shape["group"]
    tensors = mesh.shape["tensor"]
    chips = groups // 2
    half = chips // 2
    partner = [(i, i ^ 1) for i in range(groups)]
    same_core = [[2 * chip + core for chip in range(chips)] for core in range(2)]
    near = [
        [
            (2 * chip + core) * tensors + (pair * 2 + ((chip // half) ^ side))
            for chip in range(chips)
        ]
        for core in range(2)
        for pair in range(tensors // 2)
        for side in range(2)
    ]

    def body(
        hidden, norm_gain, slab_of, w_query, w_key, w_value, w_out, k_cache, v_cache, lengths
    ):
        sequences, width = hidden.shape
        slab = width // groups
        head_dim = k_cache.shape[3]
        heads = w_query.shape[1] // head_dim
        columns = w_query.shape[1] + w_key.shape[1] + w_value.shape[1]
        core = (lax.axis_index("group") % 2).reshape(1)
        other_query, other_key, other_value, other_out = (
            lax.ppermute(w, "group", partner) for w in (w_query, w_key, w_value, w_out)
        )
        lines = sequences * 2 * slab // LANES
        arranged, cosine, sine, near_query, near_key, near_value = call(
            arrange,
            (
                pltpu.VMEM((chips, lines, LANES), NARROW),
                pltpu.VMEM((sequences, head_dim), WIDE),
                pltpu.VMEM((sequences, head_dim), WIDE),
                *(pltpu.VMEM(w.shape, NARROW) for w in (w_query, w_key, w_value)),
            ),
            (core,),
            (),
            [
                pltpu.SMEM((groups,), jnp.int32),
                pltpu.SMEM((sequences,), jnp.int32),
                pltpu.VMEM((sequences, width), NARROW),
                pltpu.VMEM((1, width), WIDE),
                pltpu.VMEM((chips * lines, LANES), WIDE),
                pltpu.SemaphoreType.DMA((7,)),
            ],
            (hidden, norm_gain.reshape(1, width), slab_of, lengths, w_query, w_key, w_value),
            slab=slab,
        )
        features = exchange(arranged, ("group", "tensor"), near)
        features, other_query, other_key, other_value, other_out = lax.optimization_barrier(
            (features, other_query, other_key, other_value, other_out)
        )
        partial = call(
            project,
            pltpu.VMEM((chips, sequences, columns), WIDE),
            (),
            (
                features,
                near_query, *in_vmem(other_query), near_key, *in_vmem(other_key), near_value, *in_vmem(other_value),
            ),
            [pltpu.VMEM((chips * lines, LANES), WIDE)],
            chunk=512,
        )
        parts = exchange(partial, "group", same_core)
        attended, new_keys, new_values = call(
            attend,
            (
                pltpu.VMEM((chips, sequences * heads, head_dim), NARROW),
                jax.ShapeDtypeStruct((sequences, head_dim), NARROW),
                jax.ShapeDtypeStruct((sequences, head_dim), NARROW),
            ),
            (lengths,),
            (parts, cosine, sine, *in_vmem(k_cache, v_cache)),
            [pltpu.VMEM((sequences, heads + 8, head_dim), WIDE)],
            heads=heads,
        )
        gathered = exchange(attended, "group", same_core)
        head_partial = call(
            project_out,
            pltpu.VMEM((chips, lines, LANES), NARROW),
            (),
            (gathered, *in_vmem(w_out, other_out)),
            [
                pltpu.VMEM((chips * sequences * heads, head_dim), WIDE),
                pltpu.VMEM((chips * lines, LANES), WIDE),
            ],
            heads=heads,
        )
        returned = exchange(head_partial, "group", same_core)
        copies = call(repeat, pltpu.VMEM((tensors, chips, lines, LANES), NARROW), (), (returned,))
        everyone = lax.all_to_all(copies, "tensor", 0, 0, tiled=True)
        out_hidden = call(
            finish,
            jax.ShapeDtypeStruct((sequences, width), NARROW),
            (core, slab_of),
            (everyone, hidden),
            [pltpu.VMEM((chips * lines, LANES), WIDE)],
            slab=slab,
        )
        return (
            out_hidden,
            new_keys.reshape(sequences, 1, head_dim),
            new_values.reshape(sequences, 1, head_dim),
        )

    in_specs = (
        P("group", None),
        P(),
        P(),
        P("group", "tensor"),
        P("group", "tensor"),
        P("group", "tensor"),
        P("tensor", "group"),
        P("group", "tensor", None, None),
        P("group", "tensor", None, None),
        P("group"),
    )
    out_specs = (P("group", None), P("group", "tensor", None), P("group", "tensor", None))
    return jax.shard_map(body, mesh=mesh, in_specs=in_specs, out_specs=out_specs, check_vma=False)
```

```python
import functools
import math

import jax
import jax.numpy as jnp
from jax import lax
from jax.experimental import pallas as pl
from jax.experimental.pallas import tpu as pltpu
from jax.sharding import PartitionSpec as P

ROTARY_BASE = 500000.0
EPSILON = 1e-05
LANES = 128
WIDE = jnp.float32
NARROW = jnp.bfloat16


def in_vmem(*arrays):
    return [pltpu.with_memory_space_constraint(a, pltpu.VMEM) for a in arrays]


def in_hbm(*arrays):
    return [pltpu.with_memory_space_constraint(a, pltpu.HBM) for a in arrays]


def call(kernel, outs, scalars, arrays, scratch=(), far=(), **sizes):
    def at(space, operands):
        return [pl.BlockSpec(memory_space=space)] * len(operands)

    return pl.pallas_call(
        functools.partial(kernel, **sizes),
        out_shape=outs,
        in_specs=at(pltpu.SMEM, scalars) + at(pltpu.HBM, far) + at(pltpu.VMEM, arrays),
        out_specs=jax.tree.map(lambda _: pl.BlockSpec(memory_space=pltpu.VMEM), outs),
        scratch_shapes=list(scratch),
        compiler_params=pltpu.CompilerParams(vmem_limit_bytes=8 * 1024 * 1024),
        name=kernel.__name__,
    )(*scalars, *in_hbm(*far), *arrays)


def arrange(core_ref, *refs, slab):
    far, refs = refs[:7], refs[7:]
    out_ref, cos_ref, sin_ref, kept_ref, length_ref, slab_ref, hidden_ref, gain_ref, rows_ref, sems = refs
    near = [length_ref, slab_ref, hidden_ref, gain_ref]
    offset = 0
    for weight in far[4:]:
        near.append(kept_ref.at[:, offset : offset + weight.shape[1]])
        offset += weight.shape[1]
    copies = [pltpu.make_async_copy(f, n, sems.at[i]) for i, (f, n) in enumerate(zip(far, near))]
    for copy in copies:
        copy.start()
    sequences, width = hidden_ref.shape
    head_dim = cos_ref.shape[1]
    core = core_ref[0]
    lane = lax.broadcasted_iota(jnp.int32, (sequences, head_dim), 1)
    half_dim = head_dim // 2
    place_in_half = jnp.where(lane < half_dim, lane, lane - half_dim).astype(WIDE)
    frequency = jnp.exp(-math.log(ROTARY_BASE) * (2.0 * place_in_half) / head_dim)
    copies[0].wait()
    row = lax.broadcasted_iota(jnp.int32, (sequences, head_dim), 0)
    position = jnp.full((sequences, head_dim), length_ref[0], jnp.int32)
    for s in range(1, sequences):
        position = jnp.where(row == s, length_ref[s], position)
    angle = position.astype(WIDE) * frequency
    sine = jnp.sin(angle)
    cos_ref[...] = jnp.cos(angle)
    sin_ref[...] = jnp.where(lane < half_dim, -sine, sine)
    for copy in copies[1:4]:
        copy.wait()
    squares = jnp.zeros((sequences, slab), WIDE)
    for first in range(0, width, slab):
        x = hidden_ref[:, first : first + slab].astype(WIDE)
        squares = squares + x * x
    scale = lax.rsqrt(jnp.sum(squares, axis=1, keepdims=True) / width + EPSILON)
    chips, lines = out_ref.shape[:2]
    pieces = slab // LANES
    for chip in range(chips):
        for place in range(2):
            index = 2 * chip + (core if place == 0 else 1 - core)
            first = pl.multiple_of(slab_ref[index] * slab, slab)
            x = hidden_ref[:, pl.ds(first, slab)].astype(WIDE)
            x = x * scale * gain_ref[:, pl.ds(first, slab)]
            for piece in range(pieces):
                line = chip * lines + place * pieces + piece
                rows_ref[pl.ds(line, sequences, stride=lines // sequences), :] = x[
                    :, piece * LANES : (piece + 1) * LANES
                ]
    for chip in range(chips):
        out_ref[chip] = rows_ref[chip * lines : (chip + 1) * lines, :].astype(NARROW)
    for copy in copies[4:]:
        copy.wait()


def rows_of(x_ref, wide_ref, pieces):
    sources, lines = x_ref.shape[:2]
    for source in range(sources):
        wide_ref[source * lines : (source + 1) * lines, :] = x_ref[source].astype(WIDE)
    rows = sources * lines // pieces
    return jnp.concatenate(
        [wide_ref[pl.ds(p, rows, stride=pieces), :].astype(NARROW) for p in range(pieces)], axis=1
    )


def project(x_ref, w_ref, other_ref, out_ref, wide_ref, *, chunk):
    depth, width = w_ref.shape
    x = rows_of(x_ref, wide_ref, 2 * depth // LANES)
    own, other = x[:, :depth], x[:, depth:]
    chips, rows = out_ref.shape[:2]
    for first in range(0, width, chunk):
        last = min(first + chunk, width)
        part = jnp.dot(own, w_ref[:, first:last], preferred_element_type=WIDE)
        part += jnp.dot(other, other_ref[:, first:last], preferred_element_type=WIDE)
        for chip in range(chips):
            out_ref[chip, :, first:last] = part[chip * rows : (chip + 1) * rows]


def attend(
    length_ref, part_ref, cos_ref, sin_ref, k_ref, v_ref, out_ref, key_ref, value_ref, heads_ref,
    *, heads
):
    sequences = part_ref.shape[1]
    head_dim = k_ref.shape[3]
    cached = k_ref.shape[2]
    total = part_ref[0]
    for source in range(1, part_ref.shape[0]):
        total = total + part_ref[source]
    for s in range(sequences):
        for h in range(heads + 2):
            heads_ref[s, h : h + 1, :] = total[s : s + 1, h * head_dim : (h + 1) * head_dim]
    value_ref[...] = total[:, (heads + 1) * head_dim :].astype(NARROW)
    scaled, new_keys, own_scores = [], [], []
    for s in range(sequences):
        cosine, sine = cos_ref[s : s + 1], sin_ref[s : s + 1]

        def rotate(x):
            return x * cosine + pltpu.roll(x, head_dim // 2, 1) * sine

        query = (rotate(heads_ref[s, :heads, :]) / math.sqrt(head_dim)).astype(NARROW)
        new_key = rotate(heads_ref[s, heads : heads + 1, :]).astype(NARROW).astype(WIDE)
        scaled.append(query)
        new_keys.append(new_key)
        own_scores.append(jnp.sum(query.astype(WIDE) * new_key, axis=1, keepdims=True))
    key_ref[...] = jnp.concatenate(new_keys, axis=0).astype(NARROW)
    nothing = jnp.zeros((heads, head_dim), NARROW)
    queries = jnp.concatenate(
        [
            jnp.concatenate([q if i == s else nothing for i in range(sequences)], axis=1)
            for s, q in enumerate(scaled)
        ],
        axis=0,
    )
    keys = jnp.concatenate([k_ref[s, 0] for s in range(sequences)], axis=1)
    scores = lax.dot_general(
        queries, keys, (((1,), (1,)), ((), ())), preferred_element_type=WIDE
    )
    weights, own_weights = [], []
    for s in range(sequences):
        visible = lax.broadcasted_iota(jnp.int32, (heads, cached), 1) < length_ref[s]
        masked = jnp.where(visible, scores[s * heads : (s + 1) * heads], -1e30)
        highest = jnp.maximum(jnp.max(masked, axis=1, keepdims=True), own_scores[s])
        exponent = jnp.where(visible, jnp.exp(masked - highest), 0.0)
        own_exp = jnp.exp(own_scores[s] - highest)
        share = 1.0 / (jnp.sum(exponent, axis=1, keepdims=True) + own_exp)
        weights.append((exponent * share).astype(NARROW))
        own_weights.append((own_exp * share).astype(NARROW))
    values = jnp.concatenate([v_ref[s, 0] for s in range(sequences)], axis=1)
    combined = jnp.dot(jnp.concatenate(weights, axis=0), values, preferred_element_type=WIDE)
    for s in range(sequences):
        new_value = heads_ref[s, heads + 1 : heads + 2, :].astype(NARROW)
        mixed = combined[s * heads : (s + 1) * heads, s * head_dim : (s + 1) * head_dim]
        mixed = mixed + own_weights[s].astype(WIDE) * new_value.astype(WIDE)
        attended = mixed.astype(NARROW)
        for target in range(out_ref.shape[0]):
            out_ref[target, s * heads : (s + 1) * heads, :] = attended


def project_out(x_ref, w_ref, other_ref, out_ref, rows_ref, parts_ref, *, heads):
    chips, lines = out_ref.shape[:2]
    x = rows_of(x_ref, rows_ref, heads)
    rows = x.shape[0]
    slab = w_ref.shape[1]
    pieces = slab // LANES
    for place, w in enumerate((w_ref, other_ref)):
        part = jnp.dot(x, w[...], preferred_element_type=WIDE)
        for piece in range(pieces):
            parts_ref[pl.ds(place * pieces + piece, rows, stride=2 * pieces), :] = part[
                :, piece * LANES : (piece + 1) * LANES
            ]
    for chip in range(chips):
        out_ref[chip] = parts_ref[chip * lines : (chip + 1) * lines, :].astype(NARROW)


def repeat(x_ref, out_ref):
    for chip in range(x_ref.shape[0]):
        x = x_ref[chip]
        for target in range(out_ref.shape[0]):
            out_ref[target, chip] = x


def finish(core_ref, slab_ref, parts_ref, hidden_ref, out_ref, sums_ref, *, slab):
    core = core_ref[0]
    chips, lines = parts_ref.shape[1:3]
    sequences = hidden_ref.shape[0]
    pieces = slab // LANES
    for chip in range(chips):
        total = parts_ref[0, chip].astype(WIDE)
        for source in range(1, parts_ref.shape[0]):
            total = total + parts_ref[source, chip].astype(WIDE)
        sums_ref[chip * lines : (chip + 1) * lines, :] = total
    for chip in range(chips):
        for place in range(2):
            index = 2 * chip + (core if place == 0 else 1 - core)
            first = slab_ref[index] * slab
            for piece in range(pieces):
                line = chip * lines + place * pieces + piece
                added = sums_ref[pl.ds(line, sequences, stride=lines // sequences), :]
                at = pl.ds(pl.multiple_of(first + piece * LANES, LANES), LANES)
                out_ref[:, at] = (hidden_ref[:, at].astype(WIDE) + added).astype(NARROW)


def exchange(tiles, axis, sets):
    return lax.all_to_all(tiles, axis, 0, 0, tiled=True, axis_index_groups=sets)


def solution(mesh):
    groups = mesh.shape["group"]
    tensors = mesh.shape["tensor"]
    chips = groups // 2
    half = chips // 2
    partner = [(i, i ^ 1) for i in range(groups)]
    same_core = [[2 * chip + core for chip in range(chips)] for core in range(2)]
    near = [
        [
            (2 * chip + core) * tensors + (pair * 2 + ((chip // half) ^ side))
            for chip in range(chips)
        ]
        for core in range(2)
        for pair in range(tensors // 2)
        for side in range(2)
    ]

    def body(
        hidden, norm_gain, slab_of, w_query, w_key, w_value, w_out, k_cache, v_cache, lengths
    ):
        sequences, width = hidden.shape
        slab = width // groups
        head_dim = k_cache.shape[3]
        heads = w_query.shape[1] // head_dim
        columns = w_query.shape[1] + w_key.shape[1] + w_value.shape[1]
        core = (lax.axis_index("group") % 2).reshape(1)
        other_out = lax.ppermute(w_out, "group", partner)
        lines = sequences * 2 * slab // LANES
        arranged, cosine, sine, own_weights = call(
            arrange,
            (
                pltpu.VMEM((chips, lines, LANES), NARROW),
                pltpu.VMEM((sequences, head_dim), WIDE),
                pltpu.VMEM((sequences, head_dim), WIDE),
                pltpu.VMEM((slab, columns), NARROW),
            ),
            (core,),
            (),
            [
                pltpu.SMEM((sequences,), jnp.int32),
                pltpu.SMEM((groups,), jnp.int32),
                pltpu.VMEM((sequences, width), NARROW),
                pltpu.VMEM((1, width), WIDE),
                pltpu.VMEM((chips * lines, LANES), WIDE),
                pltpu.SemaphoreType.DMA((7,)),
            ],
            (lengths, slab_of, hidden, norm_gain.reshape(1, width), w_query, w_key, w_value),
            slab=slab,
        )
        other_weights = lax.ppermute(own_weights, "group", partner)
        features = exchange(arranged, ("group", "tensor"), near)
        features, other_weights, other_out = lax.optimization_barrier(
            (features, other_weights, other_out)
        )
        partial = call(
            project,
            pltpu.VMEM((chips, sequences, columns), WIDE),
            (),
            (features, own_weights, *in_vmem(other_weights)),
            [pltpu.VMEM((chips * lines, LANES), WIDE)],
            chunk=512,
        )
        parts = exchange(partial, "group", same_core)
        attended, new_keys, new_values = call(
            attend,
            (
                pltpu.VMEM((chips, sequences * heads, head_dim), NARROW),
                jax.ShapeDtypeStruct((sequences, head_dim), NARROW),
                jax.ShapeDtypeStruct((sequences, head_dim), NARROW),
            ),
            (lengths,),
            (parts, cosine, sine, *in_vmem(k_cache, v_cache)),
            [pltpu.VMEM((sequences, heads + 8, head_dim), WIDE)],
            heads=heads,
        )
        gathered = exchange(attended, "group", same_core)
        head_partial = call(
            project_out,
            pltpu.VMEM((chips, lines, LANES), NARROW),
            (),
            (gathered, *in_vmem(w_out, other_out)),
            [
                pltpu.VMEM((chips * sequences * heads, head_dim), WIDE),
                pltpu.VMEM((chips * lines, LANES), WIDE),
            ],
            heads=heads,
        )
        returned = exchange(head_partial, ("group", "tensor"), near)
        copies = call(repeat, pltpu.VMEM((tensors, chips, lines, LANES), NARROW), (), (returned,))
        everyone = lax.all_to_all(copies, "tensor", 0, 0, tiled=True)
        out_hidden = call(
            finish,
            jax.ShapeDtypeStruct((sequences, width), NARROW),
            (core, slab_of),
            (everyone, hidden),
            [pltpu.VMEM((chips * lines, LANES), WIDE)],
            slab=slab,
        )
        return (
            out_hidden,
            new_keys.reshape(sequences, 1, head_dim),
            new_values.reshape(sequences, 1, head_dim),
        )

    in_specs = (
        P("group", None),
        P(),
        P(),
        P("group", "tensor"),
        P("group", "tensor"),
        P("group", "tensor"),
        P("tensor", "group"),
        P("group", "tensor", None, None),
        P("group", "tensor", None, None),
        P("group"),
    )
    out_specs = (P("group", None), P("group", "tensor", None), P("group", "tensor", None))
    return jax.shard_map(body, mesh=mesh, in_specs=in_specs, out_specs=out_specs, check_vma=False)
```

```python
import functools
import math

import jax
import jax.numpy as jnp
from jax import lax
from jax.experimental import pallas as pl
from jax.experimental.pallas import tpu as pltpu
from jax.sharding import PartitionSpec as P

ROTARY_BASE = 500000.0
EPSILON = 1e-05
LANES = 128
WIDE = jnp.float32
NARROW = jnp.bfloat16


def in_vmem(*arrays):
    return [pltpu.with_memory_space_constraint(a, pltpu.VMEM) for a in arrays]


def in_hbm(*arrays):
    return [pltpu.with_memory_space_constraint(a, pltpu.HBM) for a in arrays]


def call(kernel, outs, scalars, arrays, scratch=(), far=(), **sizes):
    def at(space, operands):
        return [pl.BlockSpec(memory_space=space)] * len(operands)

    return pl.pallas_call(
        functools.partial(kernel, **sizes),
        out_shape=outs,
        in_specs=at(pltpu.SMEM, scalars) + at(pltpu.HBM, far) + at(pltpu.VMEM, arrays),
        out_specs=jax.tree.map(
            lambda out: pl.BlockSpec(
                memory_space=pltpu.SMEM if out.dtype == jnp.int32 else pltpu.VMEM
            ),
            outs,
        ),
        scratch_shapes=list(scratch),
        compiler_params=pltpu.CompilerParams(vmem_limit_bytes=8 * 1024 * 1024),
        name=kernel.__name__,
    )(*scalars, *in_hbm(*far), *arrays)


def own_core():
    return lax.rem(lax.axis_index("group"), 2)


def arrange(*refs, slab):
    far, refs = refs[:8], refs[8:]
    (
        out_ref, cos_ref, sin_ref, kept_ref, length_ref, slab_ref, hidden_ref, gain_ref, rows_ref, sems
    ) = refs
    near = [length_ref, slab_ref, hidden_ref, gain_ref]
    far = list(far)
    offset = 0
    w_out = far.pop()
    for weight in far[4:]:
        near.append(kept_ref.at[:, offset : offset + weight.shape[1]])
        offset += weight.shape[1]
    depth, columns = kept_ref.shape[0], w_out.shape[1]
    for first in range(0, w_out.shape[0], depth):
        far.append(w_out.at[first : first + depth, :])
        near.append(kept_ref.at[:, offset : offset + columns])
        offset += columns
    copies = [pltpu.make_async_copy(f, n, sems.at[i]) for i, (f, n) in enumerate(zip(far, near))]
    for copy in copies:
        copy.start()
    sequences, width = hidden_ref.shape
    head_dim = cos_ref.shape[1]
    core = own_core()
    lane = lax.broadcasted_iota(jnp.int32, (sequences, head_dim), 1)
    half_dim = head_dim // 2
    place_in_half = jnp.where(lane < half_dim, lane, lane - half_dim).astype(WIDE)
    frequency = jnp.exp(-math.log(ROTARY_BASE) * (2.0 * place_in_half) / head_dim)
    copies[0].wait()
    row = lax.broadcasted_iota(jnp.int32, (sequences, head_dim), 0)
    position = jnp.full((sequences, head_dim), length_ref[0], jnp.int32)
    for s in range(1, sequences):
        position = jnp.where(row == s, length_ref[s], position)
    angle = position.astype(WIDE) * frequency
    sine = jnp.sin(angle)
    cos_ref[...] = jnp.cos(angle)
    sin_ref[...] = jnp.where(lane < half_dim, -sine, sine)
    for copy in copies[1:4]:
        copy.wait()
    squares = jnp.zeros((sequences, slab), WIDE)
    for first in range(0, width, slab):
        x = hidden_ref[:, first : first + slab].astype(WIDE)
        squares = squares + x * x
    scale = lax.rsqrt(jnp.sum(squares, axis=1, keepdims=True) / width + EPSILON)
    chips, lines = out_ref.shape[:2]
    pieces = slab // LANES
    for chip in range(chips):
        for place in range(2):
            index = 2 * chip + (core if place == 0 else 1 - core)
            first = pl.multiple_of(slab_ref[index] * slab, slab)
            x = hidden_ref[:, pl.ds(first, slab)].astype(WIDE)
            x = x * scale * gain_ref[:, pl.ds(first, slab)]
            for piece in range(pieces):
                line = chip * lines + place * pieces + piece
                rows_ref[pl.ds(line, sequences, stride=lines // sequences), :] = x[
                    :, piece * LANES : (piece + 1) * LANES
                ]
    for chip in range(chips):
        out_ref[chip] = rows_ref[chip * lines : (chip + 1) * lines, :].astype(NARROW)
    for copy in copies[4:]:
        copy.wait()


def rows_of(x_ref, wide_ref, pieces):
    sources, lines = x_ref.shape[:2]
    for source in range(sources):
        wide_ref[source * lines : (source + 1) * lines, :] = x_ref[source].astype(WIDE)
    rows = sources * lines // pieces
    return jnp.concatenate(
        [wide_ref[pl.ds(p, rows, stride=pieces), :].astype(NARROW) for p in range(pieces)], axis=1
    )


def project(x_ref, w_ref, other_ref, out_ref, wide_ref, *, chunk):
    depth, width = w_ref.shape[0], out_ref.shape[2]
    x = rows_of(x_ref, wide_ref, 2 * depth // LANES)
    own, other = x[:, :depth], x[:, depth:]
    chips, rows = out_ref.shape[:2]
    for first in range(0, width, chunk):
        last = min(first + chunk, width)
        part = jnp.dot(own, w_ref[:, first:last], preferred_element_type=WIDE)
        part += jnp.dot(other, other_ref[:, first:last], preferred_element_type=WIDE)
        for chip in range(chips):
            out_ref[chip, :, first:last] = part[chip * rows : (chip + 1) * rows]


def attend(
    length_ref, part_ref, cos_ref, sin_ref, k_ref, v_ref, out_ref, key_ref, value_ref, heads_ref,
    *, heads
):
    sequences = part_ref.shape[1]
    head_dim = k_ref.shape[3]
    cached = k_ref.shape[2]
    total = part_ref[0]
    for source in range(1, part_ref.shape[0]):
        total = total + part_ref[source]
    for s in range(sequences):
        for h in range(heads + 2):
            heads_ref[s, h : h + 1, :] = total[s : s + 1, h * head_dim : (h + 1) * head_dim]
    value_ref[...] = total[:, (heads + 1) * head_dim :].astype(NARROW)
    scaled, new_keys, own_scores = [], [], []
    for s in range(sequences):
        cosine, sine = cos_ref[s : s + 1], sin_ref[s : s + 1]

        def rotate(x):
            return x * cosine + pltpu.roll(x, head_dim // 2, 1) * sine

        query = (rotate(heads_ref[s, :heads, :]) / math.sqrt(head_dim)).astype(NARROW)
        new_key = rotate(heads_ref[s, heads : heads + 1, :]).astype(NARROW).astype(WIDE)
        scaled.append(query)
        new_keys.append(new_key)
        own_scores.append(jnp.sum(query.astype(WIDE) * new_key, axis=1, keepdims=True))
    key_ref[...] = jnp.concatenate(new_keys, axis=0).astype(NARROW)
    nothing = jnp.zeros((heads, head_dim), NARROW)
    queries = jnp.concatenate(
        [
            jnp.concatenate([q if i == s else nothing for i in range(sequences)], axis=1)
            for s, q in enumerate(scaled)
        ],
        axis=0,
    )
    keys = jnp.concatenate([k_ref[s, 0] for s in range(sequences)], axis=1)
    scores = lax.dot_general(
        queries, keys, (((1,), (1,)), ((), ())), preferred_element_type=WIDE
    )
    weights, own_weights = [], []
    for s in range(sequences):
        visible = lax.broadcasted_iota(jnp.int32, (heads, cached), 1) < length_ref[s]
        masked = jnp.where(visible, scores[s * heads : (s + 1) * heads], -1e30)
        highest = jnp.maximum(jnp.max(masked, axis=1, keepdims=True), own_scores[s])
        exponent = jnp.where(visible, jnp.exp(masked - highest), 0.0)
        own_exp = jnp.exp(own_scores[s] - highest)
        share = 1.0 / (jnp.sum(exponent, axis=1, keepdims=True) + own_exp)
        weights.append((exponent * share).astype(NARROW))
        own_weights.append((own_exp * share).astype(NARROW))
    values = jnp.concatenate([v_ref[s, 0] for s in range(sequences)], axis=1)
    combined = jnp.dot(jnp.concatenate(weights, axis=0), values, preferred_element_type=WIDE)
    for s in range(sequences):
        new_value = heads_ref[s, heads + 1 : heads + 2, :].astype(NARROW)
        mixed = combined[s * heads : (s + 1) * heads, s * head_dim : (s + 1) * head_dim]
        mixed = mixed + own_weights[s].astype(WIDE) * new_value.astype(WIDE)
        attended = mixed.astype(NARROW)
        for target in range(out_ref.shape[0]):
            out_ref[target, s * heads : (s + 1) * heads, :] = attended


def project_out(x_ref, w_ref, other_ref, out_ref, rows_ref, parts_ref, *, heads, slab):
    chips, lines = out_ref.shape[:2]
    x = rows_of(x_ref, rows_ref, heads)
    rows, inner = x.shape
    depth, width = w_ref.shape
    offset = width - inner // depth * slab
    pieces = slab // LANES
    for place, w in enumerate((w_ref, other_ref)):
        part = jnp.zeros((rows, slab), WIDE)
        for block in range(inner // depth):
            at = offset + block * slab
            part += jnp.dot(
                x[:, block * depth : (block + 1) * depth],
                w[:, at : at + slab],
                preferred_element_type=WIDE,
            )
        for piece in range(pieces):
            parts_ref[pl.ds(place * pieces + piece, rows, stride=2 * pieces), :] = part[
                :, piece * LANES : (piece + 1) * LANES
            ]
    for chip in range(chips):
        out_ref[chip] = parts_ref[chip * lines : (chip + 1) * lines, :].astype(NARROW)


def repeat(x_ref, out_ref):
    for chip in range(x_ref.shape[0]):
        x = x_ref[chip]
        for target in range(out_ref.shape[0]):
            out_ref[target, chip] = x


def finish(
    slab_ref, parts_ref, hidden_ref, key_in, value_in, out_ref, key_ref, value_ref, sums_ref, *, slab
):
    key_ref[...] = key_in[...]
    value_ref[...] = value_in[...]
    core = own_core()
    chips, lines = parts_ref.shape[1:3]
    sequences = hidden_ref.shape[0]
    pieces = slab // LANES
    for chip in range(chips):
        total = parts_ref[0, chip].astype(WIDE)
        for source in range(1, parts_ref.shape[0]):
            total = total + parts_ref[source, chip].astype(WIDE)
        sums_ref[chip * lines : (chip + 1) * lines, :] = total
    for chip in range(chips):
        for place in range(2):
            index = 2 * chip + (core if place == 0 else 1 - core)
            first = slab_ref[index] * slab
            for piece in range(pieces):
                line = chip * lines + place * pieces + piece
                added = sums_ref[pl.ds(line, sequences, stride=lines // sequences), :]
                at = pl.ds(pl.multiple_of(first + piece * LANES, LANES), LANES)
                out_ref[:, at] = (hidden_ref[:, at].astype(WIDE) + added).astype(NARROW)


def exchange(tiles, axis, sets):
    return lax.all_to_all(tiles, axis, 0, 0, tiled=True, axis_index_groups=sets)


def solution(mesh):
    groups = mesh.shape["group"]
    tensors = mesh.shape["tensor"]
    chips = groups // 2
    half = chips // 2
    partner = [(i, i ^ 1) for i in range(groups)]
    same_core = [[2 * chip + core for chip in range(chips)] for core in range(2)]
    near = [
        [
            (2 * chip + core) * tensors + (pair * 2 + ((chip // half) ^ side))
            for chip in range(chips)
        ]
        for core in range(2)
        for pair in range(tensors // 2)
        for side in range(2)
    ]

    def body(
        hidden, norm_gain, slab_of, w_query, w_key, w_value, w_out, k_cache, v_cache, lengths
    ):
        sequences, width = hidden.shape
        slab = width // groups
        head_dim = k_cache.shape[3]
        heads = w_query.shape[1] // head_dim
        columns = w_query.shape[1] + w_key.shape[1] + w_value.shape[1]
        lines = sequences * 2 * slab // LANES
        kept = columns + w_out.shape[0] // slab * slab
        arranged, cosine, sine, own_weights, near_lengths, near_slabs = call(
            arrange,
            (
                pltpu.VMEM((chips, lines, LANES), NARROW),
                pltpu.VMEM((sequences, head_dim), WIDE),
                pltpu.VMEM((sequences, head_dim), WIDE),
                pltpu.VMEM((slab, kept), NARROW),
                pltpu.SMEM((sequences,), jnp.int32),
                pltpu.SMEM((groups,), jnp.int32),
            ),
            (),
            (),
            [
                pltpu.VMEM((sequences, width), NARROW),
                pltpu.VMEM((1, width), WIDE),
                pltpu.VMEM((chips * lines, LANES), WIDE),
                pltpu.SemaphoreType.DMA((7 + w_out.shape[0] // slab,)),
            ],
            (lengths, slab_of, hidden, norm_gain.reshape(1, width), w_query, w_key, w_value, w_out),
            slab=slab,
        )
        other_weights = lax.ppermute(own_weights, "group", partner)
        features = exchange(arranged, ("group", "tensor"), near)
        features, other_weights = lax.optimization_barrier((features, other_weights))
        other_weights, = in_vmem(other_weights)
        partial = call(
            project,
            pltpu.VMEM((chips, sequences, columns), WIDE),
            (),
            (features, own_weights, other_weights),
            [pltpu.VMEM((chips * lines, LANES), WIDE)],
            chunk=512,
        )
        parts = exchange(partial, "group", same_core)
        attended, new_keys, new_values = call(
            attend,
            (
                pltpu.VMEM((chips, sequences * heads, head_dim), NARROW),
                pltpu.VMEM((sequences, head_dim), NARROW),
                pltpu.VMEM((sequences, head_dim), NARROW),
            ),
            (near_lengths,),
            (parts, cosine, sine, *in_vmem(k_cache, v_cache)),
            [pltpu.VMEM((sequences, heads + 8, head_dim), WIDE)],
            heads=heads,
        )
        gathered = exchange(attended, "group", same_core)
        head_partial = call(
            project_out,
            pltpu.VMEM((chips, lines, LANES), NARROW),
            (),
            (gathered, own_weights, other_weights),
            [
                pltpu.VMEM((chips * sequences * heads, head_dim), WIDE),
                pltpu.VMEM((chips * lines, LANES), WIDE),
            ],
            heads=heads,
            slab=slab,
        )
        returned = exchange(head_partial, ("group", "tensor"), near)
        copies = call(repeat, pltpu.VMEM((tensors, chips, lines, LANES), NARROW), (), (returned,))
        everyone = lax.all_to_all(copies, "tensor", 0, 0, tiled=True)
        out_hidden, new_keys, new_values = call(
            finish,
            (
                jax.ShapeDtypeStruct((sequences, width), NARROW),
                jax.ShapeDtypeStruct((sequences, head_dim), NARROW),
                jax.ShapeDtypeStruct((sequences, head_dim), NARROW),
            ),
            (near_slabs,),
            (everyone, hidden, new_keys, new_values),
            [pltpu.VMEM((chips * lines, LANES), WIDE)],
            slab=slab,
        )
        return (
            out_hidden,
            new_keys.reshape(sequences, 1, head_dim),
            new_values.reshape(sequences, 1, head_dim),
        )

    in_specs = (
        P("group", None),
        P(),
        P(),
        P("group", "tensor"),
        P("group", "tensor"),
        P("group", "tensor"),
        P("tensor", "group"),
        P("group", "tensor", None, None),
        P("group", "tensor", None, None),
        P("group"),
    )
    out_specs = (P("group", None), P("group", "tensor", None), P("group", "tensor", None))
    return jax.shard_map(body, mesh=mesh, in_specs=in_specs, out_specs=out_specs, check_vma=False)
```

```python
import functools
import math

import jax
import jax.numpy as jnp
from jax import lax
from jax.experimental import pallas as pl
from jax.experimental.pallas import tpu as pltpu
from jax.sharding import PartitionSpec as P

ROTARY_BASE = 500000.0
EPSILON = 1e-05
LANES = 128
WIDE = jnp.float32
NARROW = jnp.bfloat16


def in_vmem(*arrays):
    return [pltpu.with_memory_space_constraint(a, pltpu.VMEM) for a in arrays]


def in_hbm(*arrays):
    return [pltpu.with_memory_space_constraint(a, pltpu.HBM) for a in arrays]


def call(kernel, outs, scalars, arrays, scratch=(), far=(), **sizes):
    def at(space, operands):
        return [pl.BlockSpec(memory_space=space)] * len(operands)

    return pl.pallas_call(
        functools.partial(kernel, **sizes),
        out_shape=outs,
        in_specs=at(pltpu.SMEM, scalars) + at(pltpu.HBM, far) + at(pltpu.VMEM, arrays),
        out_specs=jax.tree.map(
            lambda out: pl.BlockSpec(
                memory_space=pltpu.SMEM if out.dtype == jnp.int32 else pltpu.VMEM
            ),
            outs,
        ),
        scratch_shapes=list(scratch),
        compiler_params=pltpu.CompilerParams(vmem_limit_bytes=8 * 1024 * 1024),
        name=kernel.__name__,
    )(*scalars, *in_hbm(*far), *arrays)


def own_core():
    return lax.rem(lax.axis_index("group"), 2)


def arrange(*refs, slab):
    far, refs = refs[:8], refs[8:]
    (
        out_ref, cos_ref, sin_ref, kept_ref, length_ref, slab_ref, hidden_ref, gain_ref, rows_ref, sems
    ) = refs
    near = [length_ref, slab_ref, hidden_ref, gain_ref]
    far = list(far)
    offset = 0
    w_out = far.pop()
    for weight in far[4:]:
        near.append(kept_ref.at[:, offset : offset + weight.shape[1]])
        offset += weight.shape[1]
    depth, columns = kept_ref.shape[0], w_out.shape[1]
    for first in range(0, w_out.shape[0], depth):
        far.append(w_out.at[first : first + depth, :])
        near.append(kept_ref.at[:, offset : offset + columns])
        offset += columns
    copies = [pltpu.make_async_copy(f, n, sems.at[i]) for i, (f, n) in enumerate(zip(far, near))]
    for copy in copies:
        copy.start()
    sequences, width = hidden_ref.shape
    head_dim = cos_ref.shape[1]
    core = own_core()
    lane = lax.broadcasted_iota(jnp.int32, (sequences, head_dim), 1)
    half_dim = head_dim // 2
    place_in_half = jnp.where(lane < half_dim, lane, lane - half_dim).astype(WIDE)
    frequency = jnp.exp(-math.log(ROTARY_BASE) * (2.0 * place_in_half) / head_dim)
    copies[0].wait()
    row = lax.broadcasted_iota(jnp.int32, (sequences, head_dim), 0)
    position = jnp.full((sequences, head_dim), length_ref[0], jnp.int32)
    for s in range(1, sequences):
        position = jnp.where(row == s, length_ref[s], position)
    angle = position.astype(WIDE) * frequency
    sine = jnp.sin(angle)
    cos_ref[...] = jnp.cos(angle)
    sin_ref[...] = jnp.where(lane < half_dim, -sine, sine)
    for copy in copies[1:4]:
        copy.wait()
    squares = jnp.zeros((sequences, slab), WIDE)
    for first in range(0, width, slab):
        x = hidden_ref[:, first : first + slab].astype(WIDE)
        squares = squares + x * x
    scale = lax.rsqrt(jnp.sum(squares, axis=1, keepdims=True) / width + EPSILON)
    chips, lines = out_ref.shape[:2]
    pieces = slab // LANES
    for chip in range(chips):
        for place in range(2):
            index = 2 * chip + (core if place == 0 else 1 - core)
            first = pl.multiple_of(slab_ref[index] * slab, slab)
            x = hidden_ref[:, pl.ds(first, slab)].astype(WIDE)
            x = x * scale * gain_ref[:, pl.ds(first, slab)]
            for piece in range(pieces):
                line = chip * lines + place * pieces + piece
                rows_ref[pl.ds(line, sequences, stride=lines // sequences), :] = x[
                    :, piece * LANES : (piece + 1) * LANES
                ]
    for chip in range(chips):
        out_ref[chip] = rows_ref[chip * lines : (chip + 1) * lines, :].astype(NARROW)
    for copy in copies[4:]:
        copy.wait()


def rows_of(x_ref, wide_ref, pieces, by_sequence=False):
    sources, lines = x_ref.shape[:2]
    for source in range(sources):
        wide_ref[source * lines : (source + 1) * lines, :] = x_ref[source].astype(WIDE)
    sequences = lines // pieces
    if by_sequence:
        starts, rows, stride = [s * pieces for s in range(sequences)], sources, lines
    else:
        starts, rows, stride = [0], sources * sequences, pieces
    return jnp.concatenate(
        [
            jnp.concatenate(
                [
                    wide_ref[pl.ds(start + p, rows, stride=stride), :].astype(NARROW)
                    for p in range(pieces)
                ],
                axis=1,
            )
            for start in starts
        ],
        axis=0,
    )


def project(x_ref, w_ref, other_ref, out_ref, wide_ref, *, chunk):
    depth, width = w_ref.shape[0], out_ref.shape[2]
    x = rows_of(x_ref, wide_ref, 2 * depth // LANES)
    own, other = x[:, :depth], x[:, depth:]
    chips, rows = out_ref.shape[:2]
    for first in range(0, width, chunk):
        last = min(first + chunk, width)
        part = jnp.dot(own, w_ref[:, first:last], preferred_element_type=WIDE)
        part += jnp.dot(other, other_ref[:, first:last], preferred_element_type=WIDE)
        for chip in range(chips):
            out_ref[chip, :, first:last] = part[chip * rows : (chip + 1) * rows]


def attend(
    length_ref, part_ref, cos_ref, sin_ref, k_ref, v_ref, out_ref, key_ref, value_ref, heads_ref,
    *, heads
):
    sequences = part_ref.shape[1]
    head_dim = k_ref.shape[3]
    cached = k_ref.shape[2]
    total = part_ref[0]
    for source in range(1, part_ref.shape[0]):
        total = total + part_ref[source]
    for s in range(sequences):
        for h in range(heads + 2):
            heads_ref[s, h : h + 1, :] = total[s : s + 1, h * head_dim : (h + 1) * head_dim]
    value_ref[...] = total[:, (heads + 1) * head_dim :].astype(NARROW)
    scaled, new_keys, own_scores = [], [], []
    for s in range(sequences):
        cosine, sine = cos_ref[s : s + 1], sin_ref[s : s + 1]

        def rotate(x):
            return x * cosine + pltpu.roll(x, head_dim // 2, 1) * sine

        query = (rotate(heads_ref[s, :heads, :]) / math.sqrt(head_dim)).astype(NARROW)
        new_key = rotate(heads_ref[s, heads : heads + 1, :]).astype(NARROW).astype(WIDE)
        scaled.append(query)
        new_keys.append(new_key)
        own_scores.append(jnp.sum(query.astype(WIDE) * new_key, axis=1, keepdims=True))
    key_ref[...] = jnp.concatenate(new_keys, axis=0).astype(NARROW)
    nothing = jnp.zeros((heads, head_dim), NARROW)
    queries = jnp.concatenate(
        [
            jnp.concatenate([q if i == s else nothing for i in range(sequences)], axis=1)
            for s, q in enumerate(scaled)
        ],
        axis=0,
    )
    keys = jnp.concatenate([k_ref[s, 0] for s in range(sequences)], axis=1)
    scores = lax.dot_general(
        queries, keys, (((1,), (1,)), ((), ())), preferred_element_type=WIDE
    )
    weights, own_weights = [], []
    for s in range(sequences):
        visible = lax.broadcasted_iota(jnp.int32, (heads, cached), 1) < length_ref[s]
        masked = jnp.where(visible, scores[s * heads : (s + 1) * heads], -1e30)
        highest = jnp.maximum(jnp.max(masked, axis=1, keepdims=True), own_scores[s])
        exponent = jnp.exp(masked - highest)
        own_exp = jnp.exp(own_scores[s] - highest)
        share = 1.0 / (jnp.sum(exponent, axis=1, keepdims=True) + own_exp)
        weights.append((exponent * share).astype(NARROW))
        own_weights.append((own_exp * share).astype(NARROW))
    values = jnp.concatenate([v_ref[s, 0] for s in range(sequences)], axis=1)
    combined = jnp.dot(jnp.concatenate(weights, axis=0), values, preferred_element_type=WIDE)
    for s in range(sequences):
        new_value = heads_ref[s, heads + 1 : heads + 2, :].astype(NARROW)
        mixed = combined[s * heads : (s + 1) * heads, s * head_dim : (s + 1) * head_dim]
        mixed = mixed + own_weights[s].astype(WIDE) * new_value.astype(WIDE)
        attended = mixed.astype(NARROW)
        for target in range(out_ref.shape[0]):
            out_ref[target, s * heads : (s + 1) * heads, :] = attended


def project_out(x_ref, w_ref, other_ref, out_ref, rows_ref, parts_ref, *, heads, slab):
    chips = x_ref.shape[0]
    tiles, lines = out_ref.shape[:2]
    x = rows_of(x_ref, rows_ref, heads, by_sequence=True)
    rows, inner = x.shape
    depth, width = w_ref.shape
    offset = width - inner // depth * slab
    pieces = slab // LANES
    places = tiles // chips
    for place, w in enumerate((w_ref, other_ref)):
        part = jnp.zeros((rows, slab), WIDE)
        for block in range(inner // depth):
            at = offset + block * slab
            part += jnp.dot(
                x[:, block * depth : (block + 1) * depth],
                w[:, at : at + slab],
                preferred_element_type=WIDE,
            )
        for s in range(rows // chips):
            for piece in range(pieces):
                line = place * lines + s * pieces + piece
                parts_ref[pl.ds(line, chips, stride=places * lines), :] = part[
                    s * chips : (s + 1) * chips, piece * LANES : (piece + 1) * LANES
                ]
    for tile in range(tiles):
        out_ref[tile] = parts_ref[tile * lines : (tile + 1) * lines, :].astype(NARROW)


def join(x_ref, out_ref):
    targets, chips = out_ref.shape[:2]
    sides = x_ref.shape[0] // chips
    for chip in range(chips):
        total = x_ref[chip * sides].astype(WIDE)
        for side in range(1, sides):
            total = total + x_ref[chip * sides + side].astype(WIDE)
        total = total.astype(NARROW)
        for target in range(targets):
            out_ref[target, chip] = total


def finish(
    slab_ref, parts_ref, hidden_ref, key_in, value_in, out_ref, key_ref, value_ref, sums_ref, *, slab
):
    key_ref[...] = key_in[...]
    value_ref[...] = value_in[...]
    core = own_core()
    sources, chips, lines = parts_ref.shape[:3]
    sequences = hidden_ref.shape[0]
    pieces = slab // LANES
    places = 2
    for chip in range(chips):
        for place in range(places):
            total = parts_ref[place, chip].astype(WIDE)
            for source in range(place + places, sources, places):
                total = total + parts_ref[source, chip].astype(WIDE)
            tile = chip * places + place
            sums_ref[tile * lines : (tile + 1) * lines, :] = total
    for chip in range(chips):
        for place in range(places):
            index = 2 * chip + (core if place == 0 else 1 - core)
            first = slab_ref[index] * slab
            for piece in range(pieces):
                line = (chip * places + place) * lines + piece
                added = sums_ref[pl.ds(line, sequences, stride=pieces), :]
                at = pl.ds(pl.multiple_of(first + piece * LANES, LANES), LANES)
                out_ref[:, at] = (hidden_ref[:, at].astype(WIDE) + added).astype(NARROW)


def exchange(tiles, axis, sets):
    return lax.all_to_all(tiles, axis, 0, 0, tiled=True, axis_index_groups=sets)


def solution(mesh):
    groups = mesh.shape["group"]
    tensors = mesh.shape["tensor"]
    chips = groups // 2
    half = chips // 2
    partner = [(i, i ^ 1) for i in range(groups)]
    same_core = [[2 * chip + core for chip in range(chips)] for core in range(2)]
    near = [
        [
            (2 * chip + core) * tensors + (pair * 2 + ((chip // half) ^ side))
            for chip in range(chips)
        ]
        for core in range(2)
        for pair in range(tensors // 2)
        for side in range(2)
    ]

    columns_of_x = [
        [
            (2 * chip + core) * tensors + pair * 2 + side
            for chip in range(chips)
            for side in range(2)
        ]
        for core in range(2)
        for pair in range(tensors // 2)
    ]

    def body(
        hidden, norm_gain, slab_of, w_query, w_key, w_value, w_out, k_cache, v_cache, lengths
    ):
        sequences, width = hidden.shape
        slab = width // groups
        head_dim = k_cache.shape[3]
        heads = w_query.shape[1] // head_dim
        columns = w_query.shape[1] + w_key.shape[1] + w_value.shape[1]
        lines = sequences * 2 * slab // LANES
        kept = columns + w_out.shape[0] // slab * slab
        arranged, cosine, sine, own_weights, near_lengths, near_slabs = call(
            arrange,
            (
                pltpu.VMEM((chips, lines, LANES), NARROW),
                pltpu.VMEM((sequences, head_dim), WIDE),
                pltpu.VMEM((sequences, head_dim), WIDE),
                pltpu.VMEM((slab, kept), NARROW),
                pltpu.SMEM((sequences,), jnp.int32),
                pltpu.SMEM((groups,), jnp.int32),
            ),
            (),
            (),
            [
                pltpu.VMEM((sequences, width), NARROW),
                pltpu.VMEM((1, width), WIDE),
                pltpu.VMEM((chips * lines, LANES), WIDE),
                pltpu.SemaphoreType.DMA((7 + w_out.shape[0] // slab,)),
            ],
            (lengths, slab_of, hidden, norm_gain.reshape(1, width), w_query, w_key, w_value, w_out),
            slab=slab,
        )
        other_weights = lax.ppermute(own_weights, "group", partner)
        features = exchange(arranged, ("group", "tensor"), near)
        features, other_weights = lax.optimization_barrier((features, other_weights))
        other_weights, = in_vmem(other_weights)
        partial = call(
            project,
            pltpu.VMEM((chips, sequences, columns), WIDE),
            (),
            (features, own_weights, other_weights),
            [pltpu.VMEM((chips * lines, LANES), WIDE)],
            chunk=512,
        )
        parts = exchange(partial, "group", same_core)
        attended, new_keys, new_values = call(
            attend,
            (
                pltpu.VMEM((chips, sequences * heads, head_dim), NARROW),
                pltpu.VMEM((sequences, head_dim), NARROW),
                pltpu.VMEM((sequences, head_dim), NARROW),
            ),
            (near_lengths,),
            (parts, cosine, sine, *in_vmem(k_cache, v_cache)),
            [pltpu.VMEM((sequences, heads + 8, head_dim), WIDE)],
            heads=heads,
        )
        gathered = exchange(attended, "group", same_core)
        tile = (lines // 2, LANES)
        head_partial = call(
            project_out,
            pltpu.VMEM((2 * chips, *tile), NARROW),
            (),
            (gathered, own_weights, other_weights),
            [
                pltpu.VMEM((chips * sequences * heads, head_dim), WIDE),
                pltpu.VMEM((chips * lines, LANES), WIDE),
            ],
            heads=heads,
            slab=slab,
        )
        returned = exchange(head_partial, ("group", "tensor"), columns_of_x)
        copies = call(join, pltpu.VMEM((tensors, chips, *tile), NARROW), (), (returned,))
        everyone = lax.all_to_all(copies, "tensor", 0, 0, tiled=True)
        out_hidden, new_keys, new_values = call(
            finish,
            (
                jax.ShapeDtypeStruct((sequences, width), NARROW),
                jax.ShapeDtypeStruct((sequences, head_dim), NARROW),
                jax.ShapeDtypeStruct((sequences, head_dim), NARROW),
            ),
            (near_slabs,),
            (everyone, hidden, new_keys, new_values),
            [pltpu.VMEM((chips * lines, LANES), WIDE)],
            slab=slab,
        )
        return (
            out_hidden,
            new_keys.reshape(sequences, 1, head_dim),
            new_values.reshape(sequences, 1, head_dim),
        )

    in_specs = (
        P("group", None),
        P(),
        P(),
        P("group", "tensor"),
        P("group", "tensor"),
        P("group", "tensor"),
        P("tensor", "group"),
        P("group", "tensor", None, None),
        P("group", "tensor", None, None),
        P("group"),
    )
    out_specs = (P("group", None), P("group", "tensor", None), P("group", "tensor", None))
    return jax.shard_map(body, mesh=mesh, in_specs=in_specs, out_specs=out_specs, check_vma=False)
```

```python
import functools
import math

import jax
import jax.numpy as jnp
from jax import lax
from jax.experimental import pallas as pl
from jax.experimental.pallas import tpu as pltpu
from jax.sharding import PartitionSpec as P


ROTARY_BASE = 500000.0
EPSILON = 1e-05
LANES = 128
WIDE = jnp.float32
NARROW = jnp.bfloat16


def in_vmem(*arrays):
    return [pltpu.with_memory_space_constraint(a, pltpu.VMEM) for a in arrays]


def in_hbm(*arrays):
    return [pltpu.with_memory_space_constraint(a, pltpu.HBM) for a in arrays]


def call(kernel, outs, scalars, arrays, scratch=(), far=(), **sizes):
    def at(space, operands):
        return [pl.BlockSpec(memory_space=space)] * len(operands)

    return pl.pallas_call(
        functools.partial(kernel, **sizes),
        out_shape=outs,
        in_specs=at(pltpu.SMEM, scalars) + at(pltpu.HBM, far) + at(pltpu.VMEM, arrays),
        out_specs=jax.tree.map(
            lambda out: pl.BlockSpec(
                memory_space=pltpu.SMEM if out.dtype == jnp.int32 else pltpu.VMEM
            ),
            outs,
        ),
        scratch_shapes=list(scratch),
        compiler_params=pltpu.CompilerParams(vmem_limit_bytes=8 * 1024 * 1024),
    )(*scalars, *in_hbm(*far), *arrays)


def own_core():
    return lax.rem(lax.axis_index("group"), 2)


def arrange(*refs, slab):
    far, refs = refs[:7], refs[7:]
    (
        out_ref, cos_ref, sin_ref, kept_ref, length_ref, slab_ref, hidden_ref, gain_ref, rows_ref, sems
    ) = refs
    near = [length_ref, slab_ref, hidden_ref, gain_ref]
    offset = 0
    for weight in far[4:]:
        near.append(kept_ref.at[:, offset : offset + weight.shape[1]])
        offset += weight.shape[1]
    copies = [pltpu.make_async_copy(f, n, sems.at[i]) for i, (f, n) in enumerate(zip(far, near))]
    for copy in copies:
        copy.start()
    sequences, width = hidden_ref.shape
    head_dim = cos_ref.shape[1]
    core = own_core()
    lane = lax.broadcasted_iota(jnp.int32, (sequences, head_dim), 1)
    half_dim = head_dim // 2
    place_in_half = jnp.where(lane < half_dim, lane, lane - half_dim).astype(WIDE)
    frequency = jnp.exp(-math.log(ROTARY_BASE) * (2.0 * place_in_half) / head_dim)
    copies[0].wait()
    row = lax.broadcasted_iota(jnp.int32, (sequences, head_dim), 0)
    position = jnp.full((sequences, head_dim), length_ref[0], jnp.int32)
    for s in range(1, sequences):
        position = jnp.where(row == s, length_ref[s], position)
    angle = position.astype(WIDE) * frequency
    sine = jnp.sin(angle)
    cos_ref[...] = jnp.cos(angle)
    sin_ref[...] = jnp.where(lane < half_dim, -sine, sine)
    for copy in copies[1:4]:
        copy.wait()
    squares = jnp.zeros((sequences, slab), WIDE)
    for first in range(0, width, slab):
        x = hidden_ref[:, first : first + slab].astype(WIDE)
        squares = squares + x * x
    scale = lax.rsqrt(jnp.sum(squares, axis=1, keepdims=True) / width + EPSILON)
    chips, lines = out_ref.shape[:2]
    pieces = slab // LANES
    for chip in range(chips):
        for place in range(2):
            index = 2 * chip + (core if place == 0 else 1 - core)
            first = pl.multiple_of(slab_ref[index] * slab, slab)
            x = hidden_ref[:, pl.ds(first, slab)].astype(WIDE)
            x = x * scale * gain_ref[:, pl.ds(first, slab)]
            for piece in range(pieces):
                line = chip * lines + place * pieces + piece
                rows_ref[pl.ds(line, sequences, stride=lines // sequences), :] = x[
                    :, piece * LANES : (piece + 1) * LANES
                ]
    for chip in range(chips):
        out_ref[chip] = rows_ref[chip * lines : (chip + 1) * lines, :].astype(NARROW)
    for copy in copies[4:]:
        copy.wait()


def rows_of(x_ref, wide_ref, pieces, by_sequence=False):
    sources, lines = x_ref.shape[:2]
    for source in range(sources):
        wide_ref[source * lines : (source + 1) * lines, :] = x_ref[source].astype(WIDE)
    sequences = lines // pieces
    if by_sequence:
        starts, rows, stride = [s * pieces for s in range(sequences)], sources, lines
    else:
        starts, rows, stride = [0], sources * sequences, pieces
    return jnp.concatenate(
        [
            jnp.concatenate(
                [
                    wide_ref[pl.ds(start + p, rows, stride=stride), :].astype(NARROW)
                    for p in range(pieces)
                ],
                axis=1,
            )
            for start in starts
        ],
        axis=0,
    )


def project(x_ref, w_ref, other_ref, out_ref, wide_ref, *, chunk):
    depth, width = w_ref.shape[0], out_ref.shape[2]
    x = rows_of(x_ref, wide_ref, 2 * depth // LANES)
    own, other = x[:, :depth], x[:, depth:]
    chips, rows = out_ref.shape[:2]
    for first in range(0, width, chunk):
        last = min(first + chunk, width)
        part = jnp.dot(own, w_ref[:, first:last], preferred_element_type=WIDE)
        part += jnp.dot(other, other_ref[:, first:last], preferred_element_type=WIDE)
        for chip in range(chips):
            out_ref[chip, :, first:last] = part[chip * rows : (chip + 1) * rows]


def attend(
    length_ref, part_ref, cos_ref, sin_ref, k_ref, v_ref, out_ref, key_ref, value_ref, heads_ref,
    *, heads
):
    sequences = part_ref.shape[1]
    head_dim = k_ref.shape[3]
    cached = k_ref.shape[2]
    total = part_ref[0]
    for source in range(1, part_ref.shape[0]):
        total = total + part_ref[source]
    for s in range(sequences):
        for h in range(heads + 2):
            heads_ref[s, h : h + 1, :] = total[s : s + 1, h * head_dim : (h + 1) * head_dim]
    value_ref[...] = total[:, (heads + 1) * head_dim :].astype(NARROW)
    scaled, new_keys, own_scores = [], [], []
    for s in range(sequences):
        cosine, sine = cos_ref[s : s + 1], sin_ref[s : s + 1]

        def rotate(x):
            return x * cosine + pltpu.roll(x, head_dim // 2, 1) * sine

        query = (rotate(heads_ref[s, :heads, :]) / math.sqrt(head_dim)).astype(NARROW)
        new_key = rotate(heads_ref[s, heads : heads + 1, :]).astype(NARROW).astype(WIDE)
        scaled.append(query)
        new_keys.append(new_key)
        own_scores.append(jnp.sum(query.astype(WIDE) * new_key, axis=1, keepdims=True))
    key_ref[...] = jnp.concatenate(new_keys, axis=0).astype(NARROW)
    nothing = jnp.zeros((heads, head_dim), NARROW)
    queries = jnp.concatenate(
        [
            jnp.concatenate([q if i == s else nothing for i in range(sequences)], axis=1)
            for s, q in enumerate(scaled)
        ],
        axis=0,
    )
    keys = jnp.concatenate([k_ref[s, 0] for s in range(sequences)], axis=1)
    scores = lax.dot_general(
        queries, keys, (((1,), (1,)), ((), ())), preferred_element_type=WIDE
    )
    weights, own_weights = [], []
    for s in range(sequences):
        visible = lax.broadcasted_iota(jnp.int32, (heads, cached), 1) < length_ref[s]
        masked = jnp.where(visible, scores[s * heads : (s + 1) * heads], -1e30)
        highest = jnp.maximum(jnp.max(masked, axis=1, keepdims=True), own_scores[s])
        exponent = jnp.exp(masked - highest)
        own_exp = jnp.exp(own_scores[s] - highest)
        share = 1.0 / (jnp.sum(exponent, axis=1, keepdims=True) + own_exp)
        weights.append((exponent * share).astype(NARROW))
        own_weights.append((own_exp * share).astype(NARROW))
    values = jnp.concatenate([v_ref[s, 0] for s in range(sequences)], axis=1)
    combined = jnp.dot(jnp.concatenate(weights, axis=0), values, preferred_element_type=WIDE)
    for s in range(sequences):
        new_value = heads_ref[s, heads + 1 : heads + 2, :].astype(NARROW)
        mixed = combined[s * heads : (s + 1) * heads, s * head_dim : (s + 1) * head_dim]
        mixed = mixed + own_weights[s].astype(WIDE) * new_value.astype(WIDE)
        attended = mixed.astype(NARROW)
        for target in range(out_ref.shape[0]):
            out_ref[target, s * heads : (s + 1) * heads, :] = attended


def project_out(x_ref, w_ref, other_ref, out_ref, rows_ref, parts_ref, *, heads):
    chips = x_ref.shape[0]
    tiles, lines = out_ref.shape[:2]
    x = rows_of(x_ref, rows_ref, heads, by_sequence=True)
    rows, slab = x.shape[0], w_ref.shape[1]
    pieces = slab // LANES
    places = tiles // chips
    for place, w in enumerate((w_ref, other_ref)):
        part = jnp.dot(x, w[...], preferred_element_type=WIDE)
        for s in range(rows // chips):
            for piece in range(pieces):
                line = place * lines + s * pieces + piece
                parts_ref[pl.ds(line, chips, stride=places * lines), :] = part[
                    s * chips : (s + 1) * chips, piece * LANES : (piece + 1) * LANES
                ]
    for tile in range(tiles):
        out_ref[tile] = parts_ref[tile * lines : (tile + 1) * lines, :].astype(NARROW)


def join(x_ref, out_ref):
    targets, chips = out_ref.shape[:2]
    sides = x_ref.shape[0] // chips
    for chip in range(chips):
        total = x_ref[chip * sides].astype(WIDE)
        for side in range(1, sides):
            total = total + x_ref[chip * sides + side].astype(WIDE)
        total = total.astype(NARROW)
        for target in range(targets):
            out_ref[target, chip] = total


def finish(
    slab_ref, parts_ref, hidden_ref, key_in, value_in, out_ref, key_ref, value_ref, sums_ref, *, slab
):
    key_ref[...] = key_in[...]
    value_ref[...] = value_in[...]
    core = own_core()
    sources, chips, lines = parts_ref.shape[:3]
    sequences = hidden_ref.shape[0]
    pieces = slab // LANES
    places = 2
    for chip in range(chips):
        for place in range(places):
            total = parts_ref[place, chip].astype(WIDE)
            for source in range(place + places, sources, places):
                total = total + parts_ref[source, chip].astype(WIDE)
            tile = chip * places + place
            sums_ref[tile * lines : (tile + 1) * lines, :] = total
    for chip in range(chips):
        for place in range(places):
            index = 2 * chip + (core if place == 0 else 1 - core)
            first = slab_ref[index] * slab
            for piece in range(pieces):
                line = (chip * places + place) * lines + piece
                added = sums_ref[pl.ds(line, sequences, stride=pieces), :]
                at = pl.ds(pl.multiple_of(first + piece * LANES, LANES), LANES)
                out_ref[:, at] = (hidden_ref[:, at].astype(WIDE) + added).astype(NARROW)


def exchange(tiles, axis, sets):
    return lax.all_to_all(tiles, axis, 0, 0, tiled=True, axis_index_groups=sets)


def solution(mesh):
    groups = mesh.shape["group"]
    tensors = mesh.shape["tensor"]
    chips = groups // 2
    half = chips // 2
    partner = [(i, i ^ 1) for i in range(groups)]
    same_core = [[2 * chip + core for chip in range(chips)] for core in range(2)]
    near = [
        [
            (2 * chip + core) * tensors + (pair * 2 + ((chip // half) ^ side))
            for chip in range(chips)
        ]
        for core in range(2)
        for pair in range(tensors // 2)
        for side in range(2)
    ]

    columns_of_x = [
        [
            (2 * chip + core) * tensors + pair * 2 + side
            for chip in range(chips)
            for side in range(2)
        ]
        for core in range(2)
        for pair in range(tensors // 2)
    ]

    def body(
        hidden, norm_gain, slab_of, w_query, w_key, w_value, w_out, k_cache, v_cache, lengths
    ):
        sequences, width = hidden.shape
        slab = width // groups
        head_dim = k_cache.shape[3]
        heads = w_query.shape[1] // head_dim
        columns = w_query.shape[1] + w_key.shape[1] + w_value.shape[1]
        lines = sequences * 2 * slab // LANES
        other_out = lax.ppermute(w_out, "group", partner)
        arranged, cosine, sine, own_weights, near_lengths, near_slabs = call(
            arrange,
            (
                pltpu.VMEM((chips, lines, LANES), NARROW),
                pltpu.VMEM((sequences, head_dim), WIDE),
                pltpu.VMEM((sequences, head_dim), WIDE),
                pltpu.VMEM((slab, columns), NARROW),
                pltpu.SMEM((sequences,), jnp.int32),
                pltpu.SMEM((groups,), jnp.int32),
            ),
            (),
            (),
            [
                pltpu.VMEM((sequences, width), NARROW),
                pltpu.VMEM((1, width), WIDE),
                pltpu.VMEM((chips * lines, LANES), WIDE),
                pltpu.SemaphoreType.DMA((7,)),
            ],
            (lengths, slab_of, hidden, norm_gain.reshape(1, width), w_query, w_key, w_value),
            slab=slab,
        )
        other_weights = lax.ppermute(own_weights, "group", partner)
        features = exchange(arranged, ("group", "tensor"), near)
        features, other_weights, other_out = lax.optimization_barrier(
            (features, other_weights, other_out)
        )
        other_weights, = in_vmem(other_weights)
        partial = call(
            project,
            pltpu.VMEM((chips, sequences, columns), WIDE),
            (),
            (features, own_weights, other_weights),
            [pltpu.VMEM((chips * lines, LANES), WIDE)],
            chunk=512,
        )
        parts = exchange(partial, "group", same_core)
        parts, own_out = lax.optimization_barrier((parts, w_out))
        attended, new_keys, new_values = call(
            attend,
            (
                pltpu.VMEM((chips, sequences * heads, head_dim), NARROW),
                pltpu.VMEM((sequences, head_dim), NARROW),
                pltpu.VMEM((sequences, head_dim), NARROW),
            ),
            (near_lengths,),
            (parts, cosine, sine, *in_vmem(k_cache, v_cache)),
            [pltpu.VMEM((sequences, heads + 8, head_dim), WIDE)],
            heads=heads,
        )
        gathered = exchange(attended, "group", same_core)
        tile = (lines // 2, LANES)
        head_partial = call(
            project_out,
            pltpu.VMEM((2 * chips, *tile), NARROW),
            (),
            (gathered, *in_vmem(own_out, other_out)),
            [
                pltpu.VMEM((chips * sequences * heads, head_dim), WIDE),
                pltpu.VMEM((chips * lines, LANES), WIDE),
            ],
            heads=heads,
        )
        returned = exchange(head_partial, ("group", "tensor"), columns_of_x)
        copies = call(join, pltpu.VMEM((tensors, chips, *tile), NARROW), (), (returned,))
        everyone = lax.all_to_all(copies, "tensor", 0, 0, tiled=True)
        out_hidden, new_keys, new_values = call(
            finish,
            (
                jax.ShapeDtypeStruct((sequences, width), NARROW),
                jax.ShapeDtypeStruct((sequences, head_dim), NARROW),
                jax.ShapeDtypeStruct((sequences, head_dim), NARROW),
            ),
            (near_slabs,),
            (everyone, hidden, new_keys, new_values),
            [pltpu.VMEM((chips * lines, LANES), WIDE)],
            slab=slab,
        )
        return (
            out_hidden,
            new_keys.reshape(sequences, 1, head_dim),
            new_values.reshape(sequences, 1, head_dim),
        )

    in_specs = (
        P("group", None),
        P(),
        P(),
        P("group", "tensor"),
        P("group", "tensor"),
        P("group", "tensor"),
        P("tensor", "group"),
        P("group", "tensor", None, None),
        P("group", "tensor", None, None),
        P("group"),
    )
    out_specs = (P("group", None), P("group", "tensor", None), P("group", "tensor", None))
    return jax.shard_map(body, mesh=mesh, in_specs=in_specs, out_specs=out_specs, check_vma=False)
```

```python
import functools
import math

import jax
import jax.numpy as jnp
from jax import lax
from jax.experimental import pallas as pl
from jax.experimental.pallas import tpu as pltpu
from jax.sharding import PartitionSpec as P


ROTARY_BASE = 500000.0
EPSILON = 1e-05
LANES = 128
WIDE = jnp.float32
NARROW = jnp.bfloat16


def in_vmem(*arrays):
    return [pltpu.with_memory_space_constraint(a, pltpu.VMEM) for a in arrays]


def in_hbm(*arrays):
    return [pltpu.with_memory_space_constraint(a, pltpu.HBM) for a in arrays]


def call(kernel, outs, scalars, arrays, scratch=(), far=(), **sizes):
    def at(space, operands):
        return [pl.BlockSpec(memory_space=space)] * len(operands)

    return pl.pallas_call(
        functools.partial(kernel, **sizes),
        out_shape=outs,
        in_specs=at(pltpu.SMEM, scalars) + at(pltpu.HBM, far) + at(pltpu.VMEM, arrays),
        out_specs=jax.tree.map(
            lambda out: pl.BlockSpec(
                memory_space=pltpu.SMEM if out.dtype == jnp.int32 else pltpu.VMEM
            ),
            outs,
        ),
        scratch_shapes=list(scratch),
        compiler_params=pltpu.CompilerParams(vmem_limit_bytes=8 * 1024 * 1024),
    )(*scalars, *in_hbm(*far), *arrays)


def own_core():
    return lax.rem(lax.axis_index("group"), 2)


def arrange(*refs, slab):
    far, refs = refs[:7], refs[7:]
    (
        out_ref, cos_ref, sin_ref, kept_ref, length_ref, slab_ref, hidden_ref, gain_ref, rows_ref, sems
    ) = refs
    near = [length_ref, slab_ref, hidden_ref, gain_ref]
    offset = 0
    for weight in far[4:]:
        near.append(kept_ref.at[:, offset : offset + weight.shape[1]])
        offset += weight.shape[1]
    copies = [pltpu.make_async_copy(f, n, sems.at[i]) for i, (f, n) in enumerate(zip(far, near))]
    for copy in copies:
        copy.start()
    sequences, width = hidden_ref.shape
    head_dim = cos_ref.shape[1]
    core = own_core()
    lane = lax.broadcasted_iota(jnp.int32, (sequences, head_dim), 1)
    half_dim = head_dim // 2
    place_in_half = jnp.where(lane < half_dim, lane, lane - half_dim).astype(WIDE)
    frequency = jnp.exp(-math.log(ROTARY_BASE) * (2.0 * place_in_half) / head_dim)
    copies[0].wait()
    row = lax.broadcasted_iota(jnp.int32, (sequences, head_dim), 0)
    position = jnp.full((sequences, head_dim), length_ref[0], jnp.int32)
    for s in range(1, sequences):
        position = jnp.where(row == s, length_ref[s], position)
    angle = position.astype(WIDE) * frequency
    sine = jnp.sin(angle)
    cos_ref[...] = jnp.cos(angle)
    sin_ref[...] = jnp.where(lane < half_dim, -sine, sine)
    for copy in copies[1:4]:
        copy.wait()
    squares = jnp.zeros((sequences, slab), WIDE)
    for first in range(0, width, slab):
        x = hidden_ref[:, first : first + slab].astype(WIDE)
        squares = squares + x * x
    scale = lax.rsqrt(jnp.sum(squares, axis=1, keepdims=True) / width + EPSILON)
    chips, lines = out_ref.shape[:2]
    pieces = slab // LANES
    for chip in range(chips):
        for place in range(2):
            index = 2 * chip + (core if place == 0 else 1 - core)
            first = pl.multiple_of(slab_ref[index] * slab, slab)
            x = hidden_ref[:, pl.ds(first, slab)].astype(WIDE)
            x = x * scale * gain_ref[:, pl.ds(first, slab)]
            for piece in range(pieces):
                line = chip * lines + place * pieces + piece
                rows_ref[pl.ds(line, sequences, stride=lines // sequences), :] = x[
                    :, piece * LANES : (piece + 1) * LANES
                ]
    for chip in range(chips):
        out_ref[chip] = rows_ref[chip * lines : (chip + 1) * lines, :].astype(NARROW)
    for copy in copies[4:]:
        copy.wait()


def rows_of(x_ref, wide_ref, pieces, by_sequence=False):
    sources, lines = x_ref.shape[:2]
    for source in range(sources):
        wide_ref[source * lines : (source + 1) * lines, :] = x_ref[source].astype(WIDE)
    sequences = lines // pieces
    if by_sequence:
        starts, rows, stride = [s * pieces for s in range(sequences)], sources, lines
    else:
        starts, rows, stride = [0], sources * sequences, pieces
    return jnp.concatenate(
        [
            jnp.concatenate(
                [
                    wide_ref[pl.ds(start + p, rows, stride=stride), :].astype(NARROW)
                    for p in range(pieces)
                ],
                axis=1,
            )
            for start in starts
        ],
        axis=0,
    )


def project(x_ref, w_ref, other_ref, out_ref, wide_ref, *, chunk):
    depth, width = w_ref.shape[0], out_ref.shape[2]
    x = rows_of(x_ref, wide_ref, 2 * depth // LANES)
    own, other = x[:, :depth], x[:, depth:]
    chips, rows = out_ref.shape[:2]
    for first in range(0, width, chunk):
        last = min(first + chunk, width)
        part = jnp.dot(own, w_ref[:, first:last], preferred_element_type=WIDE)
        part += jnp.dot(other, other_ref[:, first:last], preferred_element_type=WIDE)
        for chip in range(chips):
            out_ref[chip, :, first:last] = part[chip * rows : (chip + 1) * rows]


def attend(
    length_ref, part_ref, cos_ref, sin_ref, k_ref, v_ref, out_ref, key_ref, value_ref, heads_ref,
    *, heads
):
    sequences = part_ref.shape[1]
    head_dim = k_ref.shape[3]
    cached = k_ref.shape[2]
    total = part_ref[0]
    for source in range(1, part_ref.shape[0]):
        total = total + part_ref[source]
    for s in range(sequences):
        for h in range(heads + 2):
            heads_ref[s, h : h + 1, :] = total[s : s + 1, h * head_dim : (h + 1) * head_dim]
    value_ref[...] = total[:, (heads + 1) * head_dim :].astype(NARROW)
    scaled, new_keys, own_scores = [], [], []
    for s in range(sequences):
        cosine, sine = cos_ref[s : s + 1], sin_ref[s : s + 1]

        def rotate(x):
            return x * cosine + pltpu.roll(x, head_dim // 2, 1) * sine

        query = (rotate(heads_ref[s, :heads, :]) / math.sqrt(head_dim)).astype(NARROW)
        new_key = rotate(heads_ref[s, heads : heads + 1, :]).astype(NARROW).astype(WIDE)
        scaled.append(query)
        new_keys.append(new_key)
        own_scores.append(jnp.sum(query.astype(WIDE) * new_key, axis=1, keepdims=True))
    key_ref[...] = jnp.concatenate(new_keys, axis=0).astype(NARROW)
    nothing = jnp.zeros((heads, head_dim), NARROW)
    queries = jnp.concatenate(
        [
            jnp.concatenate([q if i == s else nothing for i in range(sequences)], axis=1)
            for s, q in enumerate(scaled)
        ],
        axis=0,
    )
    step = cached // 4
    masked, highest = [], [own for own in own_scores]
    for first in range(0, cached, step):
        keys = jnp.concatenate([k_ref[s, 0, first : first + step, :] for s in range(sequences)], axis=1)
        scores = lax.dot_general(
            queries, keys, (((1,), (1,)), ((), ())), preferred_element_type=WIDE
        )
        for s in range(sequences):
            slot = lax.broadcasted_iota(jnp.int32, (heads, step), 1) + first
            seen = jnp.where(slot < length_ref[s], scores[s * heads : (s + 1) * heads], -1e30)
            masked.append(seen)
            highest[s] = jnp.maximum(highest[s], jnp.max(seen, axis=1, keepdims=True))
    exponents, shares, own_weights = [None] * len(masked), [], []
    for s in range(sequences):
        own_exp = jnp.exp(own_scores[s] - highest[s])
        total_exp = own_exp
        for i in range(s, len(masked), sequences):
            exponents[i] = jnp.exp(masked[i] - highest[s])
            total_exp = total_exp + jnp.sum(exponents[i], axis=1, keepdims=True)
        shares.append(1.0 / total_exp)
        own_weights.append((own_exp * shares[s]).astype(NARROW))
    combined = jnp.zeros((sequences * heads, sequences * head_dim), WIDE)
    for i in range(0, len(masked), sequences):
        first = i // sequences * step
        weights = jnp.concatenate(
            [(exponents[i + s] * shares[s]).astype(NARROW) for s in range(sequences)], axis=0
        )
        values = jnp.concatenate([v_ref[s, 0, first : first + step, :] for s in range(sequences)], axis=1)
        combined = combined + jnp.dot(weights, values, preferred_element_type=WIDE)
    for s in range(sequences):
        new_value = heads_ref[s, heads + 1 : heads + 2, :].astype(NARROW)
        mixed = combined[s * heads : (s + 1) * heads, s * head_dim : (s + 1) * head_dim]
        mixed = mixed + own_weights[s].astype(WIDE) * new_value.astype(WIDE)
        attended = mixed.astype(NARROW)
        for target in range(out_ref.shape[0]):
            out_ref[target, s * heads : (s + 1) * heads, :] = attended


def project_out(x_ref, w_ref, other_ref, out_ref, rows_ref, parts_ref, *, heads):
    chips = x_ref.shape[0]
    tiles, lines = out_ref.shape[:2]
    x = rows_of(x_ref, rows_ref, heads, by_sequence=True)
    rows, slab = x.shape[0], w_ref.shape[1]
    pieces = slab // LANES
    places = tiles // chips
    for place, w in enumerate((w_ref, other_ref)):
        part = jnp.dot(x, w[...], preferred_element_type=WIDE)
        for s in range(rows // chips):
            for piece in range(pieces):
                line = place * lines + s * pieces + piece
                parts_ref[pl.ds(line, chips, stride=places * lines), :] = part[
                    s * chips : (s + 1) * chips, piece * LANES : (piece + 1) * LANES
                ]
    for tile in range(tiles):
        out_ref[tile] = parts_ref[tile * lines : (tile + 1) * lines, :].astype(NARROW)


def join(x_ref, out_ref):
    targets, chips = out_ref.shape[:2]
    sides = x_ref.shape[0] // chips
    for chip in range(chips):
        total = x_ref[chip * sides].astype(WIDE)
        for side in range(1, sides):
            total = total + x_ref[chip * sides + side].astype(WIDE)
        total = total.astype(NARROW)
        for target in range(targets):
            out_ref[target, chip] = total


def finish(
    slab_ref, parts_ref, hidden_ref, key_in, value_in, out_ref, key_ref, value_ref, sums_ref, *, slab
):
    key_ref[...] = key_in[...]
    value_ref[...] = value_in[...]
    core = own_core()
    sources, chips, lines = parts_ref.shape[:3]
    sequences = hidden_ref.shape[0]
    pieces = slab // LANES
    places = 2
    for chip in range(chips):
        for place in range(places):
            total = parts_ref[place, chip].astype(WIDE)
            for source in range(place + places, sources, places):
                total = total + parts_ref[source, chip].astype(WIDE)
            tile = chip * places + place
            sums_ref[tile * lines : (tile + 1) * lines, :] = total
    for chip in range(chips):
        for place in range(places):
            index = 2 * chip + (core if place == 0 else 1 - core)
            first = slab_ref[index] * slab
            for piece in range(pieces):
                line = (chip * places + place) * lines + piece
                added = sums_ref[pl.ds(line, sequences, stride=pieces), :]
                at = pl.ds(pl.multiple_of(first + piece * LANES, LANES), LANES)
                out_ref[:, at] = (hidden_ref[:, at].astype(WIDE) + added).astype(NARROW)


def exchange(tiles, axis, sets):
    return lax.all_to_all(tiles, axis, 0, 0, tiled=True, axis_index_groups=sets)


def solution(mesh):
    groups = mesh.shape["group"]
    tensors = mesh.shape["tensor"]
    chips = groups // 2
    half = chips // 2
    partner = [(i, i ^ 1) for i in range(groups)]
    same_core = [[2 * chip + core for chip in range(chips)] for core in range(2)]
    near = [
        [
            (2 * chip + core) * tensors + (pair * 2 + ((chip // half) ^ side))
            for chip in range(chips)
        ]
        for core in range(2)
        for pair in range(tensors // 2)
        for side in range(2)
    ]

    columns_of_x = [
        [
            (2 * chip + core) * tensors + pair * 2 + side
            for chip in range(chips)
            for side in range(2)
        ]
        for core in range(2)
        for pair in range(tensors // 2)
    ]

    def body(
        hidden, norm_gain, slab_of, w_query, w_key, w_value, w_out, k_cache, v_cache, lengths
    ):
        sequences, width = hidden.shape
        slab = width // groups
        head_dim = k_cache.shape[3]
        heads = w_query.shape[1] // head_dim
        columns = w_query.shape[1] + w_key.shape[1] + w_value.shape[1]
        lines = sequences * 2 * slab // LANES
        other_out = lax.ppermute(w_out, "group", partner)
        arranged, cosine, sine, own_weights, near_lengths, near_slabs = call(
            arrange,
            (
                pltpu.VMEM((chips, lines, LANES), NARROW),
                pltpu.VMEM((sequences, head_dim), WIDE),
                pltpu.VMEM((sequences, head_dim), WIDE),
                pltpu.VMEM((slab, columns), NARROW),
                pltpu.SMEM((sequences,), jnp.int32),
                pltpu.SMEM((groups,), jnp.int32),
            ),
            (),
            (),
            [
                pltpu.VMEM((sequences, width), NARROW),
                pltpu.VMEM((1, width), WIDE),
                pltpu.VMEM((chips * lines, LANES), WIDE),
                pltpu.SemaphoreType.DMA((7,)),
            ],
            (lengths, slab_of, hidden, norm_gain.reshape(1, width), w_query, w_key, w_value),
            slab=slab,
        )
        other_weights = lax.ppermute(own_weights, "group", partner)
        features = exchange(arranged, ("group", "tensor"), near)
        features, other_weights, other_out = lax.optimization_barrier(
            (features, other_weights, other_out)
        )
        other_weights, = in_vmem(other_weights)
        partial = call(
            project,
            pltpu.VMEM((chips, sequences, columns), WIDE),
            (),
            (features, own_weights, other_weights),
            [pltpu.VMEM((chips * lines, LANES), WIDE)],
            chunk=1024,
        )
        parts = exchange(partial, "group", same_core)
        parts, own_out = lax.optimization_barrier((parts, w_out))
        attended, new_keys, new_values = call(
            attend,
            (
                pltpu.VMEM((chips, sequences * heads, head_dim), NARROW),
                pltpu.VMEM((sequences, head_dim), NARROW),
                pltpu.VMEM((sequences, head_dim), NARROW),
            ),
            (near_lengths,),
            (parts, cosine, sine, *in_vmem(k_cache, v_cache)),
            [pltpu.VMEM((sequences, heads + 8, head_dim), WIDE)],
            heads=heads,
        )
        gathered = exchange(attended, "group", same_core)
        tile = (lines // 2, LANES)
        head_partial = call(
            project_out,
            pltpu.VMEM((2 * chips, *tile), NARROW),
            (),
            (gathered, *in_vmem(own_out, other_out)),
            [
                pltpu.VMEM((chips * sequences * heads, head_dim), WIDE),
                pltpu.VMEM((chips * lines, LANES), WIDE),
            ],
            heads=heads,
        )
        returned = exchange(head_partial, ("group", "tensor"), columns_of_x)
        copies = call(join, pltpu.VMEM((tensors, chips, *tile), NARROW), (), (returned,))
        everyone = lax.all_to_all(copies, "tensor", 0, 0, tiled=True)
        out_hidden, new_keys, new_values = call(
            finish,
            (
                jax.ShapeDtypeStruct((sequences, width), NARROW),
                jax.ShapeDtypeStruct((sequences, head_dim), NARROW),
                jax.ShapeDtypeStruct((sequences, head_dim), NARROW),
            ),
            (near_slabs,),
            (everyone, hidden, new_keys, new_values),
            [pltpu.VMEM((chips * lines, LANES), WIDE)],
            slab=slab,
        )
        return (
            out_hidden,
            new_keys.reshape(sequences, 1, head_dim),
            new_values.reshape(sequences, 1, head_dim),
        )

    in_specs = (
        P("group", None),
        P(),
        P(),
        P("group", "tensor"),
        P("group", "tensor"),
        P("group", "tensor"),
        P("tensor", "group"),
        P("group", "tensor", None, None),
        P("group", "tensor", None, None),
        P("group"),
    )
    out_specs = (P("group", None), P("group", "tensor", None), P("group", "tensor", None))
    return jax.shard_map(body, mesh=mesh, in_specs=in_specs, out_specs=out_specs, check_vma=False)
```
